16 devices in a mesh: yy: 2 (over z), zz: 2 (over y), t: 4 (over x, core).
Axes of the slice: x: 2, y: 2, z: 2, core: 2. Of those that a mesh axis runs over, the one named last changes fastest.
Arguments:
- fat_links: float32 [4, 24, 128, 8, 24, 3, 3, 2], P(None, 't', 'zz', 'yy')
- long_links: float32 [4, 24, 128, 8, 24, 3, 3, 2], P(None, 't', 'zz', 'yy')
- source: float32 [24, 128, 8, 12, 3, 2], P('t', 'zz', 'yy')
- quark_mass: float32 [1], replicated
Outputs:
- output 1: float32 [24, 128, 8, 12, 3, 2], P('t', 'zz', 'yy')
- output 2: float32 [8], replicated
All inputs are finite; a program needn't handle non-finite values.
Results may differ from the reference program's by a relative error of at most 0.001.
Values are sent between devices in bfloat16 or wider.
A program may use at most 1 GiB of HBM per device.

```python
import jax
import jax.numpy as jnp
from jax import lax

T_DIM = 24
Z_DIM = 128
Y_DIM = 8
X_DIM = 24
ITERS = 8
XH_DIM = X_DIM // 2


def random_su3(base_key, site_shape):
    key_re, key_im = jax.random.split(base_key)
    raw_mat = lax.complex(jax.random.normal(key_re, site_shape + (2, 3), jnp.float32), jax.random.normal(key_im, site_shape + (2, 3), jnp.float32))
    row_one = raw_mat[..., 0, :]
    row_one = row_one / jnp.sqrt(jnp.sum(jnp.real(row_one * jnp.conj(row_one)), axis=-1, keepdims=True))
    row_two = raw_mat[..., 1, :]
    row_two = row_two - jnp.sum(jnp.conj(row_one) * row_two, axis=-1, keepdims=True) * row_one
    row_two = row_two / jnp.sqrt(jnp.sum(jnp.real(row_two * jnp.conj(row_two)), axis=-1, keepdims=True))
    row_three = jnp.conj(jnp.stack([row_one[..., 1] * row_two[..., 2] - row_one[..., 2] * row_two[..., 1], row_one[..., 2] * row_two[..., 0] - row_one[..., 0] * row_two[..., 2], row_one[..., 0] * row_two[..., 1] - row_one[..., 1] * row_two[..., 0]], axis=-1))
    su_mat = jnp.stack([row_one, row_two, row_three], axis=-2)
    return jnp.stack([jnp.real(su_mat), jnp.imag(su_mat)], axis=-1)


def setup_inputs(seed: int = 0) -> dict:
    base_key = jax.random.key(seed)
    key_fat, key_long, key_src, key_mass = jax.random.split(base_key, 4)
    site_shape = (T_DIM, Z_DIM, Y_DIM, X_DIM)
    fat_links = lax.map(lambda dir_key: random_su3(dir_key, site_shape), jax.random.split(key_fat, 4))
    long_links = 0.5 * lax.map(lambda dir_key: random_su3(dir_key, site_shape), jax.random.split(key_long, 4))
    source = jax.random.normal(key_src, (T_DIM, Z_DIM, Y_DIM, XH_DIM, 3, 2), jnp.float32)
    quark_mass = jax.random.uniform(key_mass, (1,), jnp.float32, 0.5, 1.0)
    return {'fat_links': fat_links, 'long_links': long_links, 'source': source, 'quark_mass': quark_mass}


def mat_vec(link_mat, colour_vec):
    link_re = link_mat[..., 0]
    link_im = link_mat[..., 1]
    vec_re = colour_vec[..., None, :, 0]
    vec_im = colour_vec[..., None, :, 1]
    return jnp.stack([jnp.sum(link_re * vec_re - link_im * vec_im, axis=-1), jnp.sum(link_re * vec_im + link_im * vec_re, axis=-1)], axis=-1)


def adj_vec(link_mat, colour_vec):
    link_re = link_mat[..., 0]
    link_im = link_mat[..., 1]
    vec_re = colour_vec[..., :, None, 0]
    vec_im = colour_vec[..., :, None, 1]
    return jnp.stack([jnp.sum(link_re * vec_re + link_im * vec_im, axis=-2), jnp.sum(link_re * vec_im - link_im * vec_re, axis=-2)], axis=-1)


def split_links(link_full, par_grid):
    n_dir, t_len, z_len, y_len, x_len = link_full.shape[:5]
    paired = link_full.reshape(n_dir, t_len, z_len, y_len, x_len // 2, 2, 3, 3, 2)
    par_links = par_grid[None, :, :, :, None, None, None, None]
    first_half = paired[:, :, :, :, :, 0]
    second_half = paired[:, :, :, :, :, 1]
    return jnp.where(par_links == 0, first_half, second_half), jnp.where(par_links == 0, second_half, first_half)


def xhat_shift(field_in, step_len, out_par, par_field):
    if out_par == 0:
        base_off = (step_len - 1) // 2
        odd_off = base_off + 1
    else:
        base_off = (step_len + 1) // 2
        odd_off = base_off - 1
    return jnp.where(par_field == 1, jnp.roll(field_in, -odd_off, axis=3), jnp.roll(field_in, -base_off, axis=3))


def apply_hop(psi_in, out_par, fat_out, fat_in, long_out, long_in, par_field):
    total = jnp.zeros_like(psi_in)
    for direction in range(3):
        chi_one = adj_vec(fat_in[direction], psi_in)
        chi_three = adj_vec(long_in[direction], psi_in)
        total = total + mat_vec(fat_out[direction], jnp.roll(psi_in, -1, axis=direction)) + mat_vec(long_out[direction], jnp.roll(psi_in, -3, axis=direction)) - jnp.roll(chi_one, 1, axis=direction) - jnp.roll(chi_three, 3, axis=direction)
    chi_one = adj_vec(fat_in[3], psi_in)
    chi_three = adj_vec(long_in[3], psi_in)
    total = total + mat_vec(fat_out[3], xhat_shift(psi_in, 1, out_par, par_field)) + mat_vec(long_out[3], xhat_shift(psi_in, 3, out_par, par_field)) - xhat_shift(chi_one, -1, out_par, par_field) - xhat_shift(chi_three, -3, out_par, par_field)
    return total


def reference(fat_links, long_links, source, quark_mass):
    par_grid = (jnp.arange(T_DIM)[:, None, None] + jnp.arange(Z_DIM)[None, :, None] + jnp.arange(Y_DIM)[None, None, :]) % 2
    par_field = par_grid[:, :, :, None, None, None]
    fat_even, fat_odd = split_links(fat_links, par_grid)
    long_even, long_odd = split_links(long_links, par_grid)
    mass_sq = quark_mass[0] * quark_mass[0]

    def normal_apply(vec_even):
        odd_part = apply_hop(vec_even, 1, fat_odd, fat_even, long_odd, long_even, par_field)
        return mass_sq * vec_even - apply_hop(odd_part, 0, fat_even, fat_odd, long_even, long_odd, par_field)

    src_norm = jnp.sum(source * source)

    def cg_step(carry, unused):
        sol_vec, res_vec, search_dir, res_norm = carry
        applied = normal_apply(search_dir)
        step_size = res_norm / jnp.sum(search_dir * applied)
        sol_vec = sol_vec + step_size * search_dir
        res_vec = res_vec - step_size * applied
        new_norm = jnp.sum(res_vec * res_vec)
        search_dir = res_vec + (new_norm / res_norm) * search_dir
        return (sol_vec, res_vec, search_dir, new_norm), new_norm / src_norm

    init_state = (jnp.zeros_like(source), source, source, src_norm)
    final_state, history = lax.scan(cg_step, init_state, None, length=ITERS)
    return final_state[0], history
```

```python
import jax
import jax.numpy as jnp
from jax import lax
from jax.experimental import pallas as pl
from jax.experimental.pallas import tpu as pltpu
from jax.sharding import PartitionSpec as P

MESH = pl.DeviceIdType.MESH
ITERS = 8
ROWS = 72
NV = 9
EXT = 152
F32 = jnp.float32


def cg_kernel(src_ref, mass_ref, g_hbm, sol_ref, norm_ref,
              g, fx, fy, zs, zr, pv, wv, xh_i, pz_i, red_own, red, scal,
              g_sem, send_sem, recv_sem, rsend_sem, rrecv_sem):
    yy = lax.axis_index('yy')
    zz = lax.axis_index('zz')
    tt = lax.axis_index('t')
    me = yy * 8 + zz * 4 + tt

    g_copies = [pltpu.make_async_copy(g_hbm.at[par, c], g.at[par, c], g_sem.at[par, c]) for par in (1, 0) for c in range(2)]
    for cp in g_copies:
        cp.start()

    lane = lax.broadcasted_iota(jnp.int32, (8, 128), 1)
    sub = lax.broadcasted_iota(jnp.int32, (8, 128), 0)
    zlane = lane % 64
    zslot = ((lane + 3) % 64) // 8

    def masks(i, carry):
        row = sub + i * 8
        t_row = row // 12
        xh_i[pl.ds(pl.multiple_of(i * 8, 8), 8), :] = row - t_row * 12
        pz_i[pl.ds(pl.multiple_of(i * 8, 8), 8), :] = (t_row + zlane) % 2
        return carry
    lax.fori_loop(0, NV, masks, 0)

    def halo_copies(fi, c):
        def mk(src, dst, kind, dev):
            return pltpu.make_async_remote_copy(src_ref=src, dst_ref=dst, send_sem=send_sem.at[fi, c, kind], recv_sem=recv_sem.at[fi, c, kind], device_id=dev, device_id_type=MESH)
        return [
            mk(fx.at[fi, c, :, pl.ds(40, 72), :], fy.at[fi, c], 0, (1 - yy, zz, tt)),
            mk(fx.at[fi, c, :, pl.ds(40, 40), :], fx.at[fi, c, :, pl.ds(112, 40), :], 1, (yy, zz, (tt + 3) % 4)),
            mk(fx.at[fi, c, :, pl.ds(72, 40), :], fx.at[fi, c, :, pl.ds(0, 40), :], 2, (yy, zz, (tt + 1) % 4)),
            mk(zs.at[fi, c], zr.at[fi, c], 3, (yy, 1 - zz, tt)),
        ]

    def start_halo(fi, c):
        for cp in halo_copies(fi, c):
            cp.start()

    def wait_send(fi, c):
        for cp in halo_copies(fi, c):
            cp.wait_send()

    def wait_recv(fi, c):
        for cp in halo_copies(fi, c):
            cp.wait_recv()

    def red_copy(slot, d, src_dev):
        dev = ((yy + d // 8) % 2, (zz + (d // 4) % 2) % 2, (tt + d % 4) % 4)
        return pltpu.make_async_remote_copy(src_ref=red_own.at[slot], dst_ref=red.at[slot, src_dev], send_sem=rsend_sem.at[slot, d], recv_sem=rrecv_sem.at[slot, d], device_id=dev, device_id_type=MESH)

    def red_start(slot, acc):
        red_own[slot] = acc
        for d in range(1, 16):
            red_copy(slot, d, me).start()

    def red_finish(slot):
        for d in range(1, 16):
            src_dev = ((yy + d // 8) % 2) * 8 + ((zz + (d // 4) % 2) % 2) * 4 + (tt + 4 - d % 4) % 4
            cp = red_copy(slot, d, src_dev)
            cp.wait_send()
            cp.wait_recv()
        red[slot, me] = red_own[slot]
        total = red[slot, 0]
        for d in range(1, 16):
            total = total + red[slot, d]
        total = jnp.sum(jnp.sum(total, axis=0, keepdims=True), axis=1, keepdims=True)
        return jnp.broadcast_to(total, (8, 128))

    def hop_rows(par, c, i):
        fi = 1 - par
        row = pl.multiple_of(i * 8, 8)
        acc_re = [None] * 3
        acc_im = [None] * 3

        def term(slot, vec):
            base = slot * 18
            for a in range(3):
                for b in range(3):
                    l_re = g[par, c, base + a * 6 + b * 2, pl.ds(row, 8), :]
                    l_im = g[par, c, base + a * 6 + b * 2 + 1, pl.ds(row, 8), :]
                    t_re = l_re * vec[2 * b] - l_im * vec[2 * b + 1]
                    t_im = l_re * vec[2 * b + 1] + l_im * vec[2 * b]
                    acc_re[a] = t_re if acc_re[a] is None else acc_re[a] + t_re
                    acc_im[a] = t_im if acc_im[a] is None else acc_im[a] + t_im

        def ext(off):
            return [fx[fi, c, k, pl.ds(row + (40 + off), 8), :] for k in range(6)]

        own = [fx[fi, c, k, pl.ds(row + 40, 8), :] for k in range(6)]
        xh = xh_i[pl.ds(row, 8), :]
        x_even = (pz_i[pl.ds(row, 8), :] + c + yy) % 2 == par
        term(12, own)
        lo, hi = ext(1), ext(-11)
        term(13, [jnp.where(xh == 11, h, l) for l, h in zip(lo, hi)])
        lo, hi = ext(-1), ext(11)
        term(14, [jnp.where(xh == 0, h, l) for l, h in zip(lo, hi)])
        m2, m2w, p2, p2w = ext(-2), ext(10), ext(2), ext(-10)
        term(15, [jnp.where(x_even, jnp.where(xh < 2, bw, bm), jnp.where(xh > 9, fw, fp)) for bm, bw, fp, fw in zip(m2, m2w, p2, p2w)])
        loc = [fx[fi, 1 - c, k, pl.ds(row + 40, 8), :] for k in range(6)]
        term(8, loc)
        term(9, [pltpu.roll(v, 64, 1) for v in loc])
        zpack = zr[fi, c, pl.ds(row, 8), :]
        for slot, k in ((4, 1), (5, 3)):
            term(slot, [jnp.where(zlane >= 64 - k, pltpu.roll(zpack, (64 - k - 8 * j) % 128, 1), pltpu.roll(own[j], 128 - k, 1)) for j in range(6)])
        for slot, k in ((6, 1), (7, 3)):
            term(slot, [jnp.where(zlane < k, pltpu.roll(zpack, (k + 64 - 8 * j) % 128, 1), pltpu.roll(own[j], k, 1)) for j in range(6)])
        term(0, ext(12))
        term(1, ext(36))
        term(2, ext(-12))
        term(3, ext(-36))
        rem = [fy[fi, c, k, pl.ds(row, 8), :] for k in range(6)]
        term(10, rem)
        term(11, [pltpu.roll(v, 64, 1) for v in rem])
        return [v for a in range(3) for v in (acc_re[a], acc_im[a])]

    def hop(par, c):
        def body(i, carry):
            out = hop_rows(par, c, i)
            for k in range(6):
                wv[k, pl.ds(pl.multiple_of(i * 8, 8), 8), :] = out[k]
            return carry
        lax.fori_loop(0, NV, body, 0)

    def zpack_of(vals):
        packed = vals[0]
        for j in range(1, 6):
            packed = jnp.where(zslot == j, pltpu.roll(vals[j], 8 * j, 1), packed)
        return packed

    mass = jnp.full((8, 128), mass_ref[0], F32)
    mass_sq = mass * mass
    zero = jnp.zeros((8, 128), F32)

    def init_group(c, acc):
        def body(i, acc):
            row = pl.multiple_of(i * 8, 8)
            vals = [src_ref[c, k, pl.ds(row, 8), :] for k in range(6)]
            for k in range(6):
                fx[0, c, k, pl.ds(row + 40, 8), :] = vals[k]
                fx[1, c, k, pl.ds(row + 40, 8), :] = zero
                pv[c, k, pl.ds(row, 8), :] = zero
                sol_ref[c, k, pl.ds(row, 8), :] = zero
                acc = acc + vals[k] * vals[k]
            zs[0, c, pl.ds(row, 8), :] = zpack_of(vals)
            return acc
        acc = lax.fori_loop(0, NV, body, acc)
        start_halo(0, c)
        return acc
    acc = lax.fori_loop(0, 2, init_group, zero)
    red_start(1, acc)
    rho0 = red_finish(1)
    scal[0] = rho0
    scal[1] = rho0
    scal[2] = zero
    for cp in g_copies:
        cp.wait()

    def cg_step(step, carry):
        def odd_group(c, acc):
            wait_recv(0, c)
            hop(1, c)

            @pl.when(step > 0)
            def _():
                wait_send(1, c)

            @pl.when((step > 0) & (c == 0))
            def _():
                rho = red_finish(1)
                norm_ref[pl.ds(step - 1, 1), :] = (rho / scal[0])[0:1]
                scal[2] = rho / scal[1]
                scal[1] = rho
            beta = scal[2]

            def body(i, acc):
                row = pl.multiple_of(i * 8, 8)
                vals = []
                for k in range(6):
                    s_new = wv[k, pl.ds(row, 8), :] + beta * fx[1, c, k, pl.ds(row + 40, 8), :]
                    p_new = fx[0, c, k, pl.ds(row + 40, 8), :] + beta * pv[c, k, pl.ds(row, 8), :]
                    fx[1, c, k, pl.ds(row + 40, 8), :] = s_new
                    pv[c, k, pl.ds(row, 8), :] = p_new
                    acc = acc + (s_new * s_new + mass_sq * (p_new * p_new))
                    vals.append(s_new)
                zs[1, c, pl.ds(row, 8), :] = zpack_of(vals)
                return acc
            acc = lax.fori_loop(0, NV, body, acc)
            start_halo(1, c)
            return acc
        acc = lax.fori_loop(0, 2, odd_group, zero)
        red_start(0, acc)

        def even_group(c, acc):
            wait_recv(1, c)
            hop(0, c)
            wait_send(0, c)

            @pl.when(c == 0)
            def _():
                scal[3] = scal[1] / red_finish(0)
            alpha = scal[3]

            def body(i, acc):
                row = pl.multiple_of(i * 8, 8)
                vals = []
                for k in range(6):
                    p_val = pv[c, k, pl.ds(row, 8), :]
                    q_val = mass_sq * p_val - wv[k, pl.ds(row, 8), :]
                    sol_ref[c, k, pl.ds(row, 8), :] = sol_ref[c, k, pl.ds(row, 8), :] + alpha * p_val
                    r_new = fx[0, c, k, pl.ds(row + 40, 8), :] - alpha * q_val
                    fx[0, c, k, pl.ds(row + 40, 8), :] = r_new
                    acc = acc + r_new * r_new
                    vals.append(r_new)
                zs[0, c, pl.ds(row, 8), :] = zpack_of(vals)
                return acc
            acc = lax.fori_loop(0, NV, body, acc)

            @pl.when(step < ITERS - 1)
            def _():
                start_halo(0, c)
            return acc
        acc = lax.fori_loop(0, 2, even_group, zero)
        red_start(1, acc)
        return carry
    lax.fori_loop(0, ITERS, cg_step, 0)
    rho = red_finish(1)
    norm_ref[pl.ds(ITERS - 1, 1), :] = (rho / scal[0])[0:1]

    def drain(c, carry):
        wait_send(1, c)
        return carry
    lax.fori_loop(0, 2, drain, 0)


def to_rows(field_in, flip):
    t_len, z_len, y_len, xh_len = field_in.shape[:4]
    parts = field_in.reshape(t_len, z_len, 2, 2, xh_len, 6).transpose(3, 5, 0, 4, 2, 1).reshape(2, 6, t_len * xh_len, 2 * z_len)
    return jnp.where(flip, parts[::-1], parts)


def from_rows(rows, flip, shape):
    t_len, z_len, y_len, xh_len = shape[:4]
    rows = jnp.where(flip, rows[::-1], rows)
    return rows.reshape(2, 6, t_len, xh_len, 2, z_len).transpose(2, 5, 4, 0, 3, 1).reshape(shape)


def build_links(fat, long, yy):
    n_dir, t_len, z_len, y_len, x_len = fat.shape[:5]
    xh_len = x_len // 2

    def compact(links):
        a = links.reshape(n_dir, t_len, z_len, 2, 2, xh_len, 2, 3, 3, 2)
        a = a.transpose(0, 6, 4, 7, 8, 9, 1, 5, 3, 2)
        return a.reshape(n_dir, 2, 2, 3, 3, 2, t_len, xh_len, 2 * z_len)
    v, w = compact(fat), compact(long)
    lane = jnp.arange(2 * z_len)
    h1 = lane >= z_len
    par_tz = (jnp.arange(t_len)[:, None, None] + (lane % z_len)[None, None, :]) % 2
    sign = jnp.array([-1.0, 1.0], F32)[:, None, None, None]

    def adj(m):
        return jnp.swapaxes(m, -6, -5) * sign

    swap = lambda m: jnp.roll(m, z_len, axis=-1)
    to_next_t = [(i, (i + 1) % 4) for i in range(4)]
    both = [(0, 1), (1, 0)]

    def shift_t(m, k):
        halo = lax.ppermute(m[..., t_len - k:, :, :], 't', to_next_t)
        return jnp.concatenate([halo, m[..., :t_len - k, :, :]], axis=-3)

    def shift_z(m, k):
        m = m.reshape(m.shape[:-1] + (2, z_len))
        halo = lax.ppermute(m[..., z_len - k:], 'zz', both)
        out = jnp.concatenate([halo, m[..., :z_len - k]], axis=-1)
        return out.reshape(out.shape[:-2] + (2 * z_len,))

    outs = []
    fs = []
    for par in range(2):
        f = {}
        for yp in range(2):
            xe = ((par_tz + yp) % 2) == par
            f[yp] = [(jnp.where(xe, m[mu, 0, yp], m[mu, 1, yp])) for m in (v, w) for mu in range(3)]
        fs.append(f)
    for par in range(2):
        f, o = fs[par], fs[1 - par]
        groups = []
        r_w1 = lax.ppermute(o[1][5], 'yy', both)
        r_v1 = lax.ppermute(o[1][2], 'yy', both)
        r_w0 = lax.ppermute(o[0][5], 'yy', both)
        for yp in range(2):
            xe = ((par_tz + yp) % 2) == par
            vt, vz, vy, wt, wz, wy = f[yp]
            ovt, ovz, ovy, owt, owz, owy = o[yp]
            if yp == 0:
                ls = vy
                lo = jnp.where(h1, swap(adj(o[1][2])), wy)
                rs = adj(r_w1)
                ro = jnp.where(h1, wy, swap(adj(r_v1)))
            else:
                ls = adj(o[0][2])
                lo = jnp.where(h1, swap(adj(o[0][5])), vy)
                rs = wy
                ro = jnp.where(h1, vy, swap(adj(r_w0)))
            ve, vo, we, wo = v[3, 0, yp], v[3, 1, yp], w[3, 0, yp], w[3, 1, yp]
            x0 = jnp.where(xe, ve, adj(ve))
            xp = jnp.where(xe, we, vo)
            xm = jnp.where(xe, jnp.roll(adj(vo), 1, axis=-2), jnp.roll(adj(we), 1, axis=-2))
            x2 = jnp.where(xe, jnp.roll(adj(wo), 2, axis=-2), wo)
            slots = [vt, wt, shift_t(adj(ovt), 1), shift_t(adj(owt), 3), vz, wz, shift_z(adj(ovz), 1), shift_z(adj(owz), 3), ls, lo, rs, ro, x0, xp, xm, x2]
            groups.append(jnp.stack([m.reshape(18, t_len * xh_len, 2 * z_len) for m in slots]).reshape(288, t_len * xh_len, 2 * z_len))
        grp = jnp.stack(groups)
        outs.append(jnp.where(yy == 1, grp[::-1], grp))
    return jnp.stack(outs)


def solution(mesh):
    link_spec = P(None, 't', 'zz', 'yy', None, None, None, None)
    field_spec = P('t', 'zz', 'yy', None, None, None)
    vmem = pl.BlockSpec(memory_space=pltpu.VMEM)

    def local_solve(fat_links, long_links, source, quark_mass):
        yy = lax.axis_index('yy')
        links = build_links(fat_links, long_links, yy)
        src = to_rows(source, yy == 1)
        sol, norms = pl.pallas_call(
            cg_kernel,
            out_shape=(jax.ShapeDtypeStruct((2, 6, ROWS, 128), F32), jax.ShapeDtypeStruct((8, 128), F32)),
            in_specs=[vmem, pl.BlockSpec(memory_space=pltpu.SMEM), pl.BlockSpec(memory_space=pl.ANY)],
            out_specs=(vmem, vmem),
            scratch_shapes=[
                pltpu.VMEM((2, 2, 288, ROWS, 128), F32),
                pltpu.VMEM((2, 2, 6, EXT, 128), F32),
                pltpu.VMEM((2, 2, 6, ROWS, 128), F32),
                pltpu.VMEM((2, 2, ROWS, 128), F32),
                pltpu.VMEM((2, 2, ROWS, 128), F32),
                pltpu.VMEM((2, 6, ROWS, 128), F32),
                pltpu.VMEM((6, ROWS, 128), F32),
                pltpu.VMEM((ROWS, 128), jnp.int32),
                pltpu.VMEM((ROWS, 128), jnp.int32),
                pltpu.VMEM((2, 8, 128), F32),
                pltpu.VMEM((2, 16, 8, 128), F32),
                pltpu.VMEM((4, 8, 128), F32),
                pltpu.SemaphoreType.DMA((2, 2)),
                pltpu.SemaphoreType.DMA((2, 2, 4)),
                pltpu.SemaphoreType.DMA((2, 2, 4)),
                pltpu.SemaphoreType.DMA((2, 16)),
                pltpu.SemaphoreType.DMA((2, 16)),
            ],
            compiler_params=pltpu.CompilerParams(has_side_effects=True, vmem_limit_bytes=60 * 1024 * 1024),
        )(src, quark_mass, links)
        return from_rows(sol, yy == 1, source.shape), norms[:, 0]

    return jax.shard_map(local_solve, mesh=mesh, in_specs=(link_spec, link_spec, field_spec, P(None)), out_specs=(field_spec, P()), check_vma=False)
```

```python
import jax
import jax.numpy as jnp
from jax import lax
from jax.experimental import pallas as pl
from jax.experimental.pallas import tpu as pltpu
from jax.sharding import PartitionSpec as P

MESH = pl.DeviceIdType.MESH
ITERS = 8
ROWS = 72
NV = 9
EXT = 152
F32 = jnp.float32


SUB, LANES, HALF = 8, 128, 64
BASE = 40
MATS = 18
XH = 12
STRIDE = 36
DEVS = 16
NEAR, FAR = 1, 3
PP = (2, 2)
CUTS = ('t', 'zz', 'yy')
COLS = 6


TF1, TF3, TB1, TB3, ZF1, ZF3, ZB1, ZB3, LS, LO, RS, RO, X0, XP, XM, X2 = range(16)


def flip(bit):
    return 1 - bit


def out_slot_of(mu, typ, yp):
    return {0: TF1 + typ, 1: ZF1 + typ, 2: (LS + (RO - LS) * yp, RO - yp)[typ]}[mu]


def rows8(i):
    return pl.ds(pl.multiple_of(i * SUB, SUB), SUB)


def swap_halves(v):
    return pltpu.roll(v, LANES // 2, 1)


def cg_kernel(src_ref, mass_ref, fat_ref, long_ref, sol_ref, norm_ref,
              g, fx, fy, zs, zr, pv, xv, wv, xh_i, pz_i, red_own, red, scal,
              st, dn, y_out, y_in, tv_in, tw_in, zl_out, zl_in,
              st_sem, ly_send, ly_recv, lt_send, lt_recv, lz_send, lz_recv,
              send_sem, recv_sem, rsend_sem, rrecv_sem):
    yy = lax.axis_index('yy')
    zz = lax.axis_index('zz')
    tt = lax.axis_index('t')
    me = yy * SUB + zz * 4 + tt

    raw = (fat_ref, long_ref)

    def raw_copies(mu, blk, slot):
        return [pltpu.make_async_copy(raw[typ].at[mu, blk // 2, blk % 2 + 2 * h], st.at[slot, typ, h], st_sem.at[slot, typ, h]) for typ in range(2) for h in range(2)]

    MUS = (2, 0, 1, 3)
    for cp in raw_copies(MUS[0], 0, 0):
        cp.start()

    lane = lax.broadcasted_iota(jnp.int32, (SUB, LANES), 1)
    sub = lax.broadcasted_iota(jnp.int32, (SUB, LANES), 0)
    zlane = lane % HALF
    zslot = ((lane + 3) % HALF) // SUB
    half1 = lane >= HALF

    def masks(i, carry):
        row = sub + i * SUB
        t_row = row // XH
        xh_i[rows8(i), :] = row - t_row * XH
        pz_i[rows8(i), :] = (t_row + zlane) % 2
        return carry
    lax.fori_loop(0, NV, masks, 0)

    def halo_copies(fi, c):
        def mk(src, dst, kind, dev):
            return pltpu.make_async_remote_copy(src_ref=src, dst_ref=dst, send_sem=send_sem.at[fi, c, kind], recv_sem=recv_sem.at[fi, c, kind], device_id=dev, device_id_type=MESH)
        return [
            mk(fx.at[fi, c, :, pl.ds(BASE, ROWS), :], fy.at[fi, c], 0, (flip(yy), zz, tt)),
            mk(fx.at[fi, c, :, pl.ds(BASE, BASE), :], fx.at[fi, c, :, pl.ds(112, BASE), :], 1, (yy, zz, (tt + 3) % 4)),
            mk(fx.at[fi, c, :, pl.ds(ROWS, BASE), :], fx.at[fi, c, :, pl.ds(0, BASE), :], 2, (yy, zz, (tt + 1) % 4)),
            mk(zs.at[fi, c], zr.at[fi, c], 3, (yy, flip(zz), tt)),
        ]

    def start_halo(fi, c):
        for cp in halo_copies(fi, c):
            cp.start()

    def wait_send(fi, c):
        for cp in halo_copies(fi, c):
            cp.wait_send()

    def wait_recv(fi, c):
        for cp in halo_copies(fi, c):
            cp.wait_recv()

    def red_copy(slot, d, src_dev):
        dev = ((yy + d // SUB) % 2, (zz + (d // 4) % 2) % 2, (tt + d % 4) % 4)
        return pltpu.make_async_remote_copy(src_ref=red_own.at[slot], dst_ref=red.at[slot, src_dev], send_sem=rsend_sem.at[slot, d], recv_sem=rrecv_sem.at[slot, d], device_id=dev, device_id_type=MESH)

    def red_start(slot, acc):
        red_own[slot] = acc
        for d in range(1, 16):
            red_copy(slot, d, me).start()

    def red_finish(slot):
        for d in range(1, 16):
            src_dev = ((yy + d // SUB) % 2) * SUB + ((zz + (d // 4) % 2) % 2) * 4 + (tt + 4 - d % 4) % 4
            cp = red_copy(slot, d, src_dev)
            cp.wait_send()
            cp.wait_recv()
        red[slot, me] = red_own[slot]
        total = red[slot, 0]
        for d in range(1, 16):
            total = total + red[slot, d]
        total = jnp.sum(jnp.sum(total, axis=0, keepdims=True), axis=1, keepdims=True)
        return jnp.broadcast_to(total, (SUB, LANES))

    def hop_rows(par, c, i):
        fi = flip(par)
        row = pl.multiple_of(i * SUB, SUB)
        acc_re = [None] * 3
        acc_im = [None] * 3

        def term(slot, vec):
            base = slot * MATS
            for a in range(3):
                for b in range(3):
                    l_re = g[par, c, base + a * COLS + b * 2, pl.ds(row, SUB), :]
                    l_im = g[par, c, base + a * COLS + b * 2 + 1, pl.ds(row, SUB), :]
                    t_re = l_re * vec[2 * b] - l_im * vec[2 * b + 1]
                    t_im = l_re * vec[2 * b + 1] + l_im * vec[2 * b]
                    acc_re[a] = t_re if acc_re[a] is None else acc_re[a] + t_re
                    acc_im[a] = t_im if acc_im[a] is None else acc_im[a] + t_im

        def ext(off):
            return [fx[fi, c, k, pl.ds(row + (BASE + off), SUB), :] for k in range(COLS)]

        own = [fx[fi, c, k, pl.ds(row + BASE, SUB), :] for k in range(COLS)]
        xh = xh_i[pl.ds(row, SUB), :]
        x_even = (pz_i[pl.ds(row, SUB), :] + c + yy) % 2 == par
        term(X0, own)
        lo, hi = ext(1), ext(-11)
        term(XP, [jnp.where(xh == 11, h, l) for l, h in zip(lo, hi)])
        lo, hi = ext(-1), ext(11)
        term(XM, [jnp.where(xh == 0, h, l) for l, h in zip(lo, hi)])
        m2, m2w, p2, p2w = ext(-2), ext(10), ext(2), ext(-10)
        term(X2, [jnp.where(x_even, jnp.where(xh < 2, bw, bm), jnp.where(xh > 9, fw, fp)) for bm, bw, fp, fw in zip(m2, m2w, p2, p2w)])
        loc = [fx[fi, flip(c), k, pl.ds(row + BASE, SUB), :] for k in range(COLS)]
        term(LS, loc)
        term(LO, [pltpu.roll(v, HALF, 1) for v in loc])
        zpack = zr[fi, c, pl.ds(row, SUB), :]
        for slot, k in ((ZF1, NEAR), (ZF3, FAR)):
            term(slot, [jnp.where(zlane >= HALF - k, pltpu.roll(zpack, (HALF - k - SUB * j) % LANES, 1), pltpu.roll(own[j], LANES - k, 1)) for j in range(COLS)])
        for slot, k in ((ZB1, NEAR), (ZB3, FAR)):
            term(slot, [jnp.where(zlane < k, pltpu.roll(zpack, (k + HALF - SUB * j) % LANES, 1), pltpu.roll(own[j], k, 1)) for j in range(COLS)])
        term(TF1, ext(XH))
        term(TF3, ext(FAR * XH))
        term(TB1, ext(-XH))
        term(TB3, ext(-FAR * XH))
        rem = [fy[fi, c, k, pl.ds(row, SUB), :] for k in range(COLS)]
        term(RS, rem)
        term(RO, [pltpu.roll(v, HALF, 1) for v in rem])
        return [v for a in range(3) for v in (acc_re[a], acc_im[a])]

    def hop(par, c):
        def body(i, carry):
            out = hop_rows(par, c, i)
            for k in range(COLS):
                wv[k, rows8(i), :] = out[k]
            return carry
        lax.fori_loop(0, NV, body, 0)

    def zpack_of(vals):
        packed = vals[0]
        for j in range(1, COLS):
            packed = jnp.where(zslot == j, pltpu.roll(vals[j], SUB * j, 1), packed)
        return packed

    mass = jnp.full((SUB, LANES), mass_ref[0], F32)
    mass_sq = mass * mass
    zero = jnp.zeros((SUB, LANES), F32)

    def split_src(blk, carry):
        t, yp = blk // 2, blk % 2
        c = (yp + yy) % 2
        for i in range(9):
            dn[0, SUB * i:SUB * i + SUB, :] = jnp.concatenate([src_ref[t, yp, SUB * i:SUB * i + SUB, :], src_ref[t, yp + 2, SUB * i:SUB * i + SUB, :]], axis=1)
        for k in range(COLS):
            fx[0, c, k, pl.ds(t * XH + BASE, SUB), :] = dn[0, pl.ds(k, SUB, stride=COLS), :]
            fx[0, c, k, pl.ds(t * XH + 48, 4), :] = dn[0, pl.ds(k + 48, 4, stride=COLS), :]
        return carry
    lax.fori_loop(0, XH, split_src, 0)

    def init_group(c, acc):
        def body(i, acc):
            row = pl.multiple_of(i * SUB, SUB)
            vals = [fx[0, c, k, pl.ds(row + BASE, SUB), :] for k in range(COLS)]
            for k in range(COLS):
                fx[1, c, k, pl.ds(row + BASE, SUB), :] = zero
                pv[c, k, pl.ds(row, SUB), :] = zero
                xv[c, k, pl.ds(row, SUB), :] = zero
                acc = acc + vals[k] * vals[k]
            zs[0, c, pl.ds(row, SUB), :] = zpack_of(vals)
            return acc
        acc = lax.fori_loop(0, NV, body, acc)
        start_halo(0, c)
        return acc
    acc = lax.fori_loop(0, 2, init_group, zero)
    red_start(1, acc)

    c0, c1 = yy, flip(yy)
    sign = (-1.0, 1.0)
    comps = [(a * COLS + b * 2 + ri, b * COLS + a * 2 + ri, ri) for a in range(3) for b in range(3) for ri in range(2)]

    def mat(par, c, slot, comp, rows):
        return g[par, c, slot * MATS + comp, rows, :]

    def densify(slot, wrap):
        def body(i, carry):
            for u in range(27):
                row = pl.multiple_of(i * (27 * SUB) + u * SUB, SUB)
                for typ in range(2):
                    dn[typ, pl.ds(row + ROWS, SUB), :] = jnp.concatenate([st[slot, typ, 0, pl.ds(row, SUB), :], st[slot, typ, 1, pl.ds(row, SUB), :]], axis=1)
            return carry
        lax.fori_loop(0, 2, body, 0)
        if wrap:
            for typ in range(2):
                dn[typ, :ROWS, :] = dn[typ, COLS * ROWS:, :]

    def compact(order):
        mu = MUS[order]

        def block(blk, carry):
            slot = blk % 2
            t, yp = blk // 2, blk % 2
            c = (yp + yy) % 2

            @pl.when(blk < 11)
            def _():
                for cp in raw_copies(mu, blk + 1, flip(slot)):
                    cp.start()
            if order < 3:
                @pl.when(blk == 11)
                def _():
                    for cp in raw_copies(MUS[order + 1], 0, flip(slot)):
                        cp.start()
            for cp in raw_copies(mu, blk, slot):
                cp.wait()
            densify(slot, mu == 3)
            for off, n in ((0, SUB), (SUB, 4)):
                even = (t + yp + zlane[:n]) % 2 == 0

                def piece(typ, xpar, comp, back=0):
                    return dn[typ, pl.ds(ROWS + xpar * MATS + comp + STRIDE * (off - back), n, stride=STRIDE), :]

                def put(out_slot, comp, par, val):
                    g[par, c, out_slot * MATS + comp, pl.ds(t * XH + off, n), :] = val
                for comp, adj, ri in comps:
                    if mu != 3:
                        for typ in range(2):
                            out_slot = out_slot_of(mu, typ, yp)
                            e, o = piece(typ, 0, comp), piece(typ, 1, comp)
                            put(out_slot, comp, 0, jnp.where(even, e, o))
                            put(out_slot, comp, 1, jnp.where(even, o, e))
                    else:
                        pairs = (
                            (X0, piece(0, 0, comp), sign[ri] * piece(0, 0, adj)),
                            (XP, piece(1, 0, comp), piece(0, 1, comp)),
                            (XM, sign[ri] * piece(0, 1, adj, 1), sign[ri] * piece(1, 0, adj, 1)),
                            (X2, sign[ri] * piece(1, 1, adj, 2), piece(1, 1, comp)),
                        )
                        for out_slot, e, o in pairs:
                            put(out_slot, comp, 0, jnp.where(even, e, o))
                            put(out_slot, comp, 1, jnp.where(even, o, e))
            return carry
        lax.fori_loop(0, XH, block, 0)

    def ly_copies(par):
        dev = (flip(yy), zz, tt)
        return [
            pltpu.make_async_remote_copy(src_ref=g.at[flip(par), c1, pl.ds(RS * MATS, MATS)], dst_ref=g.at[par, c1, pl.ds(RS * MATS, MATS)], send_sem=ly_send.at[par, 0], recv_sem=ly_recv.at[par, 0], device_id=dev, device_id_type=MESH),
            pltpu.make_async_remote_copy(src_ref=y_out.at[par], dst_ref=y_in.at[par], send_sem=ly_send.at[par, 1], recv_sem=ly_recv.at[par, 1], device_id=dev, device_id_type=MESH),
        ]

    def ly_arrivals(par):
        dev = (flip(yy), zz, tt)
        return [
            pltpu.make_async_remote_copy(src_ref=g.at[flip(par), c1, pl.ds(RS * MATS, MATS)], dst_ref=g.at[par, c0, pl.ds(RS * MATS, MATS)], send_sem=ly_send.at[par, 0], recv_sem=ly_recv.at[par, 0], device_id=dev, device_id_type=MESH),
            pltpu.make_async_remote_copy(src_ref=y_out.at[par], dst_ref=y_in.at[par], send_sem=ly_send.at[par, 1], recv_sem=ly_recv.at[par, 1], device_id=dev, device_id_type=MESH),
        ]

    def lt_copies():
        dev = (yy, zz, (tt + 1) % 4)
        out = []
        for par in range(2):
            for c in range(2):
                out.append(pltpu.make_async_remote_copy(src_ref=g.at[flip(par), c, pl.ds(0, MATS), pl.ds(56, 16), :], dst_ref=tv_in.at[par, c], send_sem=lt_send.at[par, c, 0], recv_sem=lt_recv.at[par, c, 0], device_id=dev, device_id_type=MESH))
                out.append(pltpu.make_async_remote_copy(src_ref=g.at[flip(par), c, pl.ds(MATS, MATS), pl.ds(32, BASE), :], dst_ref=tw_in.at[par, c], send_sem=lt_send.at[par, c, 1], recv_sem=lt_recv.at[par, c, 1], device_id=dev, device_id_type=MESH))
        return out

    def lz_copy():
        return pltpu.make_async_remote_copy(src_ref=zl_out, dst_ref=zl_in, send_sem=lz_send, recv_sem=lz_recv, device_id=(yy, flip(zz), tt), device_id_type=MESH)

    compact(0)
    for par in (1, 0):
        def y_pack(i, carry):
            rows = rows8(i)
            v1 = [swap_halves(mat(flip(par), c1, RO, comp, rows)) for comp in range(MATS)]
            for comp in range(MATS):
                y_out[par, comp, rows, :] = jnp.where(half1, mat(flip(par), c0, RO, comp, rows), v1[comp])
            return carry
        lax.fori_loop(0, NV, y_pack, 0)
        for cp in ly_copies(par):
            cp.start()

    compact(1)
    for cp in lt_copies():
        cp.start()

    compact(2)

    def z_pack(n, carry):
        par, c = n // 2, n % 2

        def body(i, carry):
            rows = rows8(i)
            for typ in range(2):
                for third in range(3):
                    zl_out[par, c, typ, third, rows, :] = zpack_of([g[flip(par), c, (4 + typ) * MATS + third * COLS + j, rows, :] for j in range(COLS)])
            return carry
        lax.fori_loop(0, NV, body, 0)
        return carry
    lax.fori_loop(0, 4, z_pack, 0)
    lz_copy().start()

    compact(3)

    for par in (1, 0):
        def y_local(i, carry):
            rows = rows8(i)
            for src_c, own_c in ((c1, c0), (c0, c1)):
                far = [swap_halves(mat(flip(par), src_c, RO, adj, rows)) for comp, adj, ri in comps]
                own = [mat(par, own_c, RO, comp, rows) for comp in range(MATS)]
                for comp, adj, ri in comps:
                    g[par, own_c, LO * MATS + comp, rows, :] = jnp.where(half1, sign[ri] * far[comp], own[comp])
            v0 = [mat(flip(par), c0, LS, adj, rows) for comp, adj, ri in comps]
            for comp, adj, ri in comps:
                g[par, c1, LS * MATS + comp, rows, :] = sign[ri] * v0[comp]
            return carry
        lax.fori_loop(0, NV, y_local, 0)

    for cp in lt_copies():
        cp.wait_send()
        cp.wait_recv()

    def t_back(n, carry):
        par, c = n // 2, n % 2

        def move(slot, dst, load, src):
            for off, cnt in ((0, SUB), (SUB, 4)):
                for comp, adj, ri in comps:
                    g[par, c, slot * MATS + comp, pl.ds(dst + off, cnt), :] = sign[ri] * load(adj, pl.ds(src + off, cnt))

        def v_local(q, carry):
            move(TB1, XH * q + XH, lambda k, rows: g[flip(par), c, k, rows, :], XH * q)
            return carry
        lax.fori_loop(0, 5, v_local, 0)
        move(TB1, 0, lambda k, rows: tv_in[par, c, k, rows, :], 4)

        def w_all(q, carry):
            move(TB3, XH * q + STRIDE, lambda k, rows: g[flip(par), c, MATS + k, rows, :], XH * q)
            move(TB3, XH * q, lambda k, rows: tw_in[par, c, k, rows, :], XH * q + 4)
            return carry
        lax.fori_loop(0, 3, w_all, 0)
        return carry
    lax.fori_loop(0, 4, t_back, 0)

    lz_copy().wait_send()
    lz_copy().wait_recv()

    def z_back(n, carry):
        par, c = n // 2, n % 2

        def body(i, carry):
            rows = rows8(i)
            for typ, k in ((0, NEAR), (1, FAR)):
                packs = [zl_in[par, c, typ, third, rows, :] for third in range(3)]
                back = []
                for comp, adj, ri in comps:
                    own = pltpu.roll(mat(flip(par), c, 4 + typ, adj, rows), k, 1)
                    far = pltpu.roll(packs[adj // COLS], (k + HALF - SUB * (adj % COLS)) % LANES, 1)
                    back.append(sign[ri] * jnp.where(zlane < k, far, own))
                for comp, val in enumerate(back):
                    g[par, c, (COLS + typ) * MATS + comp, rows, :] = val
            return carry
        lax.fori_loop(0, NV, body, 0)
        return carry
    lax.fori_loop(0, 4, z_back, 0)

    for par in (1, 0):
        for cp in ly_copies(par):
            cp.wait_send()
    for par in (1, 0):
        for cp in ly_arrivals(par):
            cp.wait_recv()

        def y_far(i, carry):
            rows = rows8(i)
            w1 = [mat(par, c0, RS, comp, rows) for comp in range(MATS)]
            for comp, adj, ri in comps:
                g[par, c0, RS * MATS + comp, rows, :] = sign[ri] * w1[adj]
            far = [sign[ri] * y_in[par, adj, rows, :] for comp, adj, ri in comps]
            swapped = [swap_halves(v) for v in far]
            for c, vals in ((c0, far), (c1, swapped)):
                own = [mat(par, c, RO, comp, rows) for comp in range(MATS)]
                for comp in range(MATS):
                    g[par, c, RO * MATS + comp, rows, :] = jnp.where(half1, own[comp], vals[comp])
            return carry
        lax.fori_loop(0, NV, y_far, 0)

    rho0 = red_finish(1)
    scal[0] = rho0
    scal[1] = rho0
    scal[2] = zero

    def cg_step(step, carry):
        def odd_group(c, acc):
            wait_recv(0, c)
            hop(1, c)

            @pl.when(step > 0)
            def _():
                wait_send(1, c)

            @pl.when((step > 0) & (c == 0))
            def _():
                rho = red_finish(1)
                norm_ref[pl.ds(step - 1, 1), :] = (rho / scal[0])[0:1]
                scal[2] = rho / scal[1]
                scal[1] = rho
            beta = scal[2]

            def body(n, acc):
                packs = []
                for u in range(3):
                    rows, ext = rows8(n * 3 + u), rows8(n * 3 + u + 5)
                    vals = []
                    for k in range(COLS):
                        s_new = wv[k, rows, :] + beta * fx[1, c, k, ext, :]
                        p_new = fx[0, c, k, ext, :] + beta * pv[c, k, rows, :]
                        fx[1, c, k, ext, :] = s_new
                        pv[c, k, rows, :] = p_new
                        acc = acc + (s_new * s_new + mass_sq * (p_new * p_new))
                        vals.append(s_new)
                    packs.append((rows, zpack_of(vals)))
                for rows, pack in packs:
                    zs[1, c, rows, :] = pack
                return acc
            acc = lax.fori_loop(0, 3, body, acc)

            @pl.when(c == 1)
            def _():
                red_start(0, acc)
            start_halo(1, c)
            return acc
        lax.fori_loop(0, 2, odd_group, zero)

        def even_group(c, acc):
            wait_recv(1, c)
            hop(0, c)
            wait_send(0, c)

            @pl.when(c == 0)
            def _():
                scal[3] = scal[1] / red_finish(0)
            alpha = scal[3]

            def body(n, acc):
                packs = []
                for u in range(3):
                    rows, ext = rows8(n * 3 + u), rows8(n * 3 + u + 5)
                    vals = []
                    for k in range(COLS):
                        p_val = pv[c, k, rows, :]
                        q_val = mass_sq * p_val - wv[k, rows, :]
                        xv[c, k, rows, :] = xv[c, k, rows, :] + alpha * p_val
                        r_new = fx[0, c, k, ext, :] - alpha * q_val
                        fx[0, c, k, ext, :] = r_new
                        acc = acc + r_new * r_new
                        vals.append(r_new)
                    packs.append((rows, zpack_of(vals)))
                for rows, pack in packs:
                    zs[0, c, rows, :] = pack
                return acc
            acc = lax.fori_loop(0, 3, body, acc)

            @pl.when(c == 1)
            def _():
                red_start(1, acc)

            @pl.when(step < ITERS - 1)
            def _():
                start_halo(0, c)
            return acc
        lax.fori_loop(0, 2, even_group, zero)
        return carry
    lax.fori_loop(0, ITERS, cg_step, 0)
    rho = red_finish(1)
    norm_ref[pl.ds(ITERS - 1, 1), :] = (rho / scal[0])[0:1]

    def drain(c, carry):
        wait_send(1, c)
        return carry
    lax.fori_loop(0, 2, drain, 0)

    def join_sol(blk, carry):
        t, yp = blk // 2, blk % 2
        c = (yp + yy) % 2
        for k in range(COLS):
            dn[0, pl.ds(k, SUB, stride=COLS), :] = xv[c, k, pl.ds(t * XH, SUB), :]
            dn[0, pl.ds(k + 48, 4, stride=COLS), :] = xv[c, k, pl.ds(t * XH + SUB, 4), :]
        for i in range(9):
            val = dn[0, SUB * i:SUB * i + SUB, :]
            sol_ref[t, yp, SUB * i:SUB * i + SUB, :] = val[:, :HALF]
            sol_ref[t, yp + 2, SUB * i:SUB * i + SUB, :] = pltpu.roll(val, HALF, 1)[:, :HALF]
        return carry
    lax.fori_loop(0, XH, join_sol, 0)


def solution(mesh):
    link_spec = P(None, *CUTS)
    field_spec = P(*CUTS)
    vmem = pl.BlockSpec(memory_space=pltpu.VMEM)

    def local_solve(fat_links, long_links, source, quark_mass):
        t_len, z_len, y_len, xh_len = source.shape[:4]

        def link_rows(links):
            return jnp.moveaxis(links, 2, -1).reshape(4, t_len, y_len, STRIDE * xh_len, z_len)
        src = jnp.moveaxis(source, 1, -1).reshape(t_len, y_len, COLS * xh_len, z_len)
        hbm = pl.BlockSpec(memory_space=pl.ANY)
        dma = pltpu.SemaphoreType.DMA
        sol, norms = pl.pallas_call(
            cg_kernel,
            out_shape=(jax.ShapeDtypeStruct(src.shape, F32), jax.ShapeDtypeStruct((SUB, LANES), F32)),
            in_specs=[vmem, pl.BlockSpec(memory_space=pltpu.SMEM), hbm, hbm],
            out_specs=(vmem, vmem),
            scratch_shapes=[
                pltpu.VMEM(PP + (288, ROWS, LANES), F32),
                pltpu.VMEM(PP + (COLS, EXT, LANES), F32),
                pltpu.VMEM(PP + (COLS, ROWS, LANES), F32),
                pltpu.VMEM(PP + (ROWS, LANES), F32),
                pltpu.VMEM(PP + (ROWS, LANES), F32),
                pltpu.VMEM((2, COLS, ROWS, LANES), F32),
                pltpu.VMEM((2, COLS, ROWS, LANES), F32),
                pltpu.VMEM((COLS, ROWS, LANES), F32),
                pltpu.VMEM((ROWS, LANES), jnp.int32),
                pltpu.VMEM((ROWS, LANES), jnp.int32),
                pltpu.VMEM((2, SUB, LANES), F32),
                pltpu.VMEM((2, 16, SUB, LANES), F32),
                pltpu.VMEM((4, SUB, LANES), F32),
                pltpu.VMEM(PP + (2, STRIDE * xh_len, z_len), F32),
                pltpu.VMEM((2, 504, LANES), F32),
                pltpu.VMEM((2, MATS, ROWS, LANES), F32),
                pltpu.VMEM((2, MATS, ROWS, LANES), F32),
                pltpu.VMEM(PP + (MATS, 16, LANES), F32),
                pltpu.VMEM(PP + (MATS, BASE, LANES), F32),
                pltpu.VMEM(PP + (2, 3, ROWS, LANES), F32),
                pltpu.VMEM(PP + (2, 3, ROWS, LANES), F32),
                *[dma(PP + n) for n in ((2,), (), (), (2,), (2,))], dma, dma,
                dma(PP + (4,)), dma(PP + (4,)), dma((2, DEVS)), dma((2, DEVS)),
            ],
            compiler_params=pltpu.CompilerParams(has_side_effects=True, vmem_limit_bytes=61 * 1024 * 1024),
        )(src, quark_mass, link_rows(fat_links), link_rows(long_links))
        sol = jnp.moveaxis(sol.reshape(t_len, y_len, xh_len, 3, 2, z_len), -1, 1)
        return sol, norms[:, 0]

    return jax.shard_map(local_solve, mesh=mesh, in_specs=(link_spec, link_spec, field_spec, P()), out_specs=(field_spec, P()), check_vma=False)
```

```python
import jax
import jax.numpy as jnp
from jax import lax
from jax.experimental import pallas as pl
from jax.experimental.pallas import tpu as pltpu
from jax.sharding import PartitionSpec as P

MESH = pl.DeviceIdType.MESH
ITERS = 8
ROWS = 72
NV = 9
EXT = 152
F32 = jnp.float32


SUB, LANES, HALF = 8, 128, 64
BASE = 40
MATS = 18
XH = 12
STRIDE = 36
DEVS = 16
NEAR, FAR = 1, 3
SLOTS = 4
PP = (2, 2)
CUTS = ('t', 'zz', 'yy')
COLS = 6


TF1, TF3, TB1, TB3, ZF1, ZF3, ZB1, ZB3, LS, LO, RS, RO, X0, XP, XM, X2 = range(16)


def flip(bit):
    return 1 - bit


def out_slot_of(mu, typ, yp):
    return {0: TF1 + typ, 1: ZF1 + typ, 2: (LS + (RO - LS) * yp, RO - yp)[typ]}[mu]


def blk_t(blk):
    return blk // 2 if isinstance(blk, int) else half_of(blk)


def blk_y(blk):
    return blk % 2 if isinstance(blk, int) else mod(blk, 2)


def mod(a, n):
    return lax.rem(a, jnp.full_like(a, n))


def half_of(a):
    return lax.div(a, jnp.full_like(a, 2))


def rows8(i):
    return pl.ds(pl.multiple_of(i * SUB, SUB), SUB)


def swap_halves(v):
    return pltpu.roll(v, LANES // 2, 1)


def cg_kernel(src_ref, mass_ref, fat_ref, long_ref, sol_ref, norm_ref,
              g, fx, fy, zs, zr, pv, xv, wv, xh_i, pz_i, red_own, red, scal,
              st, dn, pw, y_out, y_in, tv_in, tw_in, zl_out, zl_in,
              st_sem, ly_send, ly_recv, lt_send, lt_recv, lz_send, lz_recv,
              send_sem, recv_sem, rsend_sem, rrecv_sem):
    yy = lax.axis_index('yy')
    zz = lax.axis_index('zz')
    tt = lax.axis_index('t')
    t_prev, t_next = mod(tt + 3, 4), mod(tt + 1, 4)
    me = yy * SUB + zz * 4 + tt

    raw = (fat_ref, long_ref)

    def raw_copies(mu, blk, slot):
        return [pltpu.make_async_copy(raw[typ].at[mu, blk_t(blk), blk_y(blk) + 2 * h], st.at[slot, typ, h], st_sem.at[slot, typ, h]) for typ in range(2) for h in range(2)]

    MUS = (2, 0, 1, 3)
    for ahead in range(SLOTS - 1):
        for cp in raw_copies(MUS[0], ahead, ahead):
            cp.start()

    lane = lax.broadcasted_iota(jnp.int32, (SUB, LANES), 1)
    sub = lax.broadcasted_iota(jnp.int32, (SUB, LANES), 0)
    zlane = lane % HALF
    zslot = ((lane + 3) % HALF) // SUB
    half1 = lane >= HALF

    def masks(i, carry):
        row = sub + i * SUB
        t_row = row // XH
        xh_i[rows8(i), :] = row - t_row * XH
        pz_i[rows8(i), :] = (t_row + zlane) % 2
        return carry
    lax.fori_loop(0, NV, masks, 0)

    def halo_copies(fi, c, kinds=range(4)):
        def mk(src, dst, kind, dev):
            return pltpu.make_async_remote_copy(src_ref=src, dst_ref=dst, send_sem=send_sem.at[fi, c, kind], recv_sem=recv_sem.at[fi, c, kind], device_id=dev, device_id_type=MESH)
        makers = (
            lambda: mk((fx.at[fi, 0, :, pl.ds(BASE, ROWS), :], pw.at[fi])[c], fy.at[fi, flip(c)], 0, (flip(yy), zz, tt)),
            lambda: mk(fx.at[fi, c, :, pl.ds(BASE, BASE), :], fx.at[fi, c, :, pl.ds(BASE + ROWS, BASE), :], 1, (yy, zz, t_prev)),
            lambda: mk(fx.at[fi, c, :, pl.ds(ROWS, BASE), :], fx.at[fi, c, :, pl.ds(0, BASE), :], 2, (yy, zz, t_next)),
            lambda: mk(zs.at[fi, c], zr.at[fi, c], 3, (yy, flip(zz), tt)),
        )
        return [makers[k]() for k in kinds]

    def start_halo(fi, c, kinds=range(4)):
        for cp in halo_copies(fi, c, kinds):
            cp.start()

    def wait_send(fi, c):
        for cp in halo_copies(fi, c):
            cp.wait_send()

    def wait_edges(fi, c):
        for cp in halo_copies(fi, c, (1, 2, 3)):
            cp.wait_recv()

    def wait_far(fi, c):
        halo_copies(fi, flip(c), (0,))[0].wait_recv()

    peers = []
    for d in range(1, DEVS):
        dev_y = flip(yy) if d // SUB else yy
        dev_z = flip(zz) if (d // 4) % 2 else zz
        dev_t = mod(tt + d % 4, 4)
        peers.append(((dev_y, dev_z, dev_t), dev_y * SUB + dev_z * 4 + mod(tt + 4 - d % 4, 4)))

    def red_copy(slot, d, src_dev):
        return pltpu.make_async_remote_copy(src_ref=red_own.at[slot], dst_ref=red.at[slot, src_dev], send_sem=rsend_sem.at[slot, d], recv_sem=rrecv_sem.at[slot, d], device_id=peers[d - 1][0], device_id_type=MESH)

    def red_start(slot, acc):
        red_own[slot] = acc
        for d in range(1, 16):
            red_copy(slot, d, me).start()

    def red_finish(slot):
        for d in range(1, 16):
            cp = red_copy(slot, d, peers[d - 1][1])
            cp.wait_send()
            cp.wait_recv()
        red[slot, me] = red_own[slot]
        total = red[slot, 0]
        for d in range(1, 16):
            total = total + red[slot, d]
        total = jnp.sum(jnp.sum(total, axis=0, keepdims=True), axis=1, keepdims=True)
        return jnp.broadcast_to(total, (SUB, LANES))

    def mat(par, c, slot, comp, rows):
        return g[par, c, slot * MATS + comp, rows, :]

    def adder(par, c, row, acc):
        def term(slot, vec):
            rows = pl.ds(row, SUB)
            for a in range(3):
                for b in range(3):
                    l_re = mat(par, c, slot, a * COLS + 2 * b, rows)
                    l_im = mat(par, c, slot, a * COLS + 2 * b + 1, rows)
                    v_re, v_im = vec[2 * b], vec[2 * b + 1]
                    for k, t in ((2 * a, l_re * v_re - l_im * v_im), (2 * a + 1, l_re * v_im + l_im * v_re)):
                        acc[k] = t if acc[k] is None else acc[k] + t
        return term

    def hop_own(par, c, i):
        fi = flip(par)
        row = pl.multiple_of(i * SUB, SUB)
        acc = [None] * COLS
        term = adder(par, c, row, acc)

        def ext(off):
            start = row + (BASE + off)
            return [fx[fi, c, k, pl.ds(start, SUB), :] for k in range(COLS)]

        own = ext(0)
        xh = xh_i[pl.ds(row, SUB), :]
        x_even = mod(pz_i[pl.ds(row, SUB), :] + c, 2) == par
        term(X0, own)
        lo, hi = ext(1), ext(-11)
        edge = xh == 11
        term(XP, [lax.select(edge, h, l) for l, h in zip(lo, hi)])
        lo, hi = ext(-1), ext(11)
        edge = xh == 0
        term(XM, [lax.select(edge, h, l) for l, h in zip(lo, hi)])
        m2, m2w, p2, p2w = ext(-2), ext(10), ext(2), ext(-10)
        low, high = xh < 2, xh > 9
        term(X2, [lax.select(x_even, lax.select(low, bw, bm), lax.select(high, fw, fp)) for bm, bw, fp, fw in zip(m2, m2w, p2, p2w)])
        mid = row + BASE
        loc = [fx[fi, flip(c), k, pl.ds(mid, SUB), :] for k in range(COLS)]
        term(LS, loc)
        term(LO, [pltpu.roll(v, HALF, 1) for v in loc])
        zpack = zr[fi, c, pl.ds(row, SUB), :]
        for slot, k in ((ZF1, NEAR), (ZF3, FAR)):
            edge = zlane >= HALF - k
            term(slot, [lax.select(edge, pltpu.roll(zpack, (HALF - k - SUB * j) % LANES, 1), pltpu.roll(own[j], LANES - k, 1)) for j in range(COLS)])
        for slot, k in ((ZB1, NEAR), (ZB3, FAR)):
            edge = zlane < k
            term(slot, [lax.select(edge, pltpu.roll(zpack, (k + HALF - SUB * j) % LANES, 1), pltpu.roll(own[j], k, 1)) for j in range(COLS)])
        term(TF1, ext(XH))
        term(TF3, ext(FAR * XH))
        term(TB1, ext(-XH))
        term(TB3, ext(-FAR * XH))
        return acc

    def hop(par, c):
        def body(i, carry):
            out = hop_own(par, c, i)
            for k in range(COLS):
                wv[k, rows8(i), :] = out[k]
            return carry
        lax.fori_loop(0, NV, body, 0)

    def across(par, c, i, vec, acc):
        term = adder(par, c, pl.multiple_of(i * SUB, SUB), acc)
        term(RS, vec)
        term(RO, [swap_halves(v) for v in vec])
        return acc

    def hop_far(par, c, i):
        rows = rows8(i)
        acc = [wv[k, rows, :] for k in range(COLS)]
        rem = [fy[flip(par), c, k, rows, :] for k in range(COLS)]
        if c == 0:
            return [a + v for a, v in zip(acc, rem)]
        return across(par, c, i, rem, acc)

    def sums_out(fi, i, vals):
        for k, v in enumerate(across(flip(fi), 0, i, vals, [None] * COLS)):
            pw[fi, k, rows8(i), :] = v

    in_slot = [zslot == j for j in range(COLS)]

    def zpack_of(vals):
        packed = vals[0]
        for j in range(1, COLS):
            packed = lax.select(in_slot[j], pltpu.roll(vals[j], SUB * j, 1), packed)
        return packed

    mass = jnp.full((SUB, LANES), mass_ref[0], F32)
    mass_sq = mass * mass
    zero = jnp.zeros((SUB, LANES), F32)

    def split_src(blk, carry):
        t, yp = half_of(blk), mod(blk, 2)
        c = yp
        for i in range(9):
            dn[0, SUB * i:SUB * i + SUB, :] = jnp.concatenate([src_ref[t, yp, SUB * i:SUB * i + SUB, :], src_ref[t, yp + 2, SUB * i:SUB * i + SUB, :]], axis=1)
        for k in range(COLS):
            fx[0, c, k, pl.ds(t * XH + BASE, SUB), :] = dn[0, pl.ds(k, SUB, stride=COLS), :]
            fx[0, c, k, pl.ds(t * XH + 48, 4), :] = dn[0, pl.ds(k + 48, 4, stride=COLS), :]
        return carry
    lax.fori_loop(0, XH, split_src, 0)

    acc = zero
    for c in range(2):
        def init_body(i, acc):
            rows, ext = rows8(i), rows8(i + 5)
            vals = [fx[0, c, k, ext, :] for k in range(COLS)]
            for k in range(COLS):
                fx[1, c, k, ext, :] = zero
                pv[c, k, rows, :] = zero
                xv[c, k, rows, :] = zero
                acc = acc + vals[k] * vals[k]
            zs[0, c, rows, :] = zpack_of(vals)
            return acc
        acc = lax.fori_loop(0, NV, init_body, acc)
        start_halo(0, c, range(c, 4))
    red_start(1, acc)

    c0, c1 = 0, 1
    sign = (-1.0, 1.0)
    comps = [(a * COLS + b * 2 + ri, b * COLS + a * 2 + ri, ri) for a in range(3) for b in range(3) for ri in range(2)]

    def densify(slot, wrap):
        def body(i, carry):
            for u in range(27):
                row = pl.multiple_of(i * (27 * SUB) + u * SUB, SUB)
                for typ in range(2):
                    dn[typ, pl.ds(row + ROWS, SUB), :] = jnp.concatenate([st[slot, typ, 0, pl.ds(row, SUB), :], st[slot, typ, 1, pl.ds(row, SUB), :]], axis=1)
            return carry
        lax.fori_loop(0, 2, body, 0)
        if wrap:
            for typ in range(2):
                dn[typ, :ROWS, :] = dn[typ, COLS * ROWS:, :]

    def base_of(slot):
        return slot * MATS

    def compact(order):
        mu = MUS[order]

        def block(blk, carry):
            slot = mod(blk, SLOTS)
            t, yp = half_of(blk), mod(blk, 2)
            c = yp
            ahead = blk + SLOTS - 1
            ahead_slot = mod(ahead, SLOTS)

            @pl.when(ahead < XH)
            def _():
                for cp in raw_copies(mu, ahead, ahead_slot):
                    cp.start()
            if order < 3:
                @pl.when(ahead >= XH)
                def _():
                    for cp in raw_copies(MUS[order + 1], ahead - XH, ahead_slot):
                        cp.start()
            for cp in raw_copies(mu, blk, slot):
                cp.wait()
            densify(slot, mu == 3)
            for off, n in ((0, SUB), (SUB, 4)):
                out_rows = pl.ds(t * XH + off, n)
                even = mod(zlane[:n] + (t + yp), 2) == 0

                def piece(typ, xpar, comp, back=0):
                    return dn[typ, pl.ds(ROWS + xpar * MATS + comp + STRIDE * (off - back), n, stride=STRIDE), :]

                def put(out_slot, comp, par, val):
                    g[par, c, base_of(out_slot) + comp, out_rows, :] = val
                for comp, adj, ri in comps:
                    if mu != 3:
                        for typ in range(2):
                            out_slot = out_slot_of(mu, typ, yp)
                            e, o = piece(typ, 0, comp), piece(typ, 1, comp)
                            put(out_slot, comp, 0, lax.select(even, e, o))
                            put(out_slot, comp, 1, lax.select(even, o, e))
                    else:
                        pairs = (
                            (X0, piece(0, 0, comp), sign[ri] * piece(0, 0, adj)),
                            (XP, piece(1, 0, comp), piece(0, 1, comp)),
                            (XM, sign[ri] * piece(0, 1, adj, 1), sign[ri] * piece(1, 0, adj, 1)),
                            (X2, sign[ri] * piece(1, 1, adj, 2), piece(1, 1, comp)),
                        )
                        for out_slot, e, o in pairs:
                            put(out_slot, comp, 0, lax.select(even, e, o))
                            put(out_slot, comp, 1, lax.select(even, o, e))
            return carry
        lax.fori_loop(0, XH, block, 0)

    def ly_copy():
        return pltpu.make_async_remote_copy(src_ref=y_out, dst_ref=y_in, send_sem=ly_send.at[0], recv_sem=ly_recv.at[0], device_id=(flip(yy), zz, tt), device_id_type=MESH)

    def lt_copies(par):
        dev = (yy, zz, t_next)
        out = []
        for c in range(2):
            out.append(pltpu.make_async_remote_copy(src_ref=g.at[flip(par), c, pl.ds(0, MATS), pl.ds(56, 16), :], dst_ref=tv_in.at[par, c], send_sem=lt_send.at[par, c, 0], recv_sem=lt_recv.at[par, c, 0], device_id=dev, device_id_type=MESH))
            out.append(pltpu.make_async_remote_copy(src_ref=g.at[flip(par), c, pl.ds(MATS, MATS), pl.ds(32, BASE), :], dst_ref=tw_in.at[par, c], send_sem=lt_send.at[par, c, 1], recv_sem=lt_recv.at[par, c, 1], device_id=dev, device_id_type=MESH))
        return out

    def lz_copy(par):
        return pltpu.make_async_remote_copy(src_ref=zl_out.at[par], dst_ref=zl_in.at[par], send_sem=lz_send.at[par], recv_sem=lz_recv.at[par], device_id=(yy, flip(zz), tt), device_id_type=MESH)

    compact(0)

    def y_pack(i, carry):
        rows = rows8(i)
        w0 = [swap_halves(mat(0, c0, RO, comp, rows)) for comp in range(MATS)]
        for comp in range(MATS):
            y_out[comp, rows, :] = lax.select(half1, mat(1, c0, RO, comp, rows), w0[comp])
        return carry
    lax.fori_loop(0, NV, y_pack, 0)
    ly_copy().start()

    compact(1)
    for par in (1, 0):
        for cp in lt_copies(par):
            cp.start()

    compact(2)

    def z_pack(n, carry):
        par, c = half_of(n), mod(n, 2)

        def body(i, carry):
            rows = rows8(i)
            for typ in range(2):
                for third in range(3):
                    zl_out[par, c, typ, third, rows, :] = zpack_of([mat(flip(par), c, ZF1 + typ, third * COLS + j, rows) for j in range(COLS)])
            return carry
        lax.fori_loop(0, NV, body, 0)
        return carry
    lax.fori_loop(0, 4, z_pack, 0)
    for par in (1, 0):
        lz_copy(par).start()

    def y_local(par, carry):
        def body(i, carry):
            rows = rows8(i)
            for src_c, own_c in ((c1, c0), (c0, c1)):
                far = [swap_halves(mat(flip(par), src_c, RO, adj, rows)) for comp, adj, ri in comps]
                own = [mat(par, own_c, RO, comp, rows) for comp in range(MATS)]
                for comp, adj, ri in comps:
                    g[par, own_c, LO * MATS + comp, rows, :] = lax.select(half1, sign[ri] * far[comp], own[comp])
            v0 = [mat(flip(par), c0, LS, adj, rows) for comp, adj, ri in comps]
            for comp, adj, ri in comps:
                g[par, c1, LS * MATS + comp, rows, :] = sign[ri] * v0[comp]
            return carry
        lax.fori_loop(0, NV, body, 0)
        return carry
    lax.fori_loop(0, 2, y_local, 0)

    def y_far(par):
        def body(i, carry):
            rows = rows8(i)
            w_in = [y_in[comp, rows, :] for comp in range(MATS)]
            if par == 0:
                w_in = [swap_halves(v) for v in w_in]
            v1 = [swap_halves(mat(flip(par), c1, RO, adj, rows)) for comp, adj, ri in comps]
            own = [mat(par, c1, RO, comp, rows) for comp in range(MATS)]
            for comp, adj, ri in comps:
                g[par, c1, RO * MATS + comp, rows, :] = lax.select(half1, own[comp], sign[ri] * w_in[adj])
                g[par, c0, RO * MATS + comp, rows, :] = lax.select(half1, w_in[comp], sign[ri] * v1[comp])
            w1 = [mat(flip(par), c1, RS, adj, rows) for comp, adj, ri in comps]
            for comp, adj, ri in comps:
                g[par, c0, RS * MATS + comp, rows, :] = sign[ri] * w1[comp]
            return carry
        lax.fori_loop(0, NV, body, 0)

    ly_copy().wait_send()
    ly_copy().wait_recv()
    y_far(1)

    def src_sums(i, carry):
        sums_out(0, i, [fx[0, 1, k, rows8(i + 5), :] for k in range(COLS)])
        return carry
    lax.fori_loop(0, NV, src_sums, 0)
    start_halo(0, 1, (0,))
    y_far(0)

    compact(3)

    for par in (1, 0):
        for cp in lt_copies(par):
            cp.wait_send()
            cp.wait_recv()

    def t_back(n, carry):
        par, c = half_of(n), mod(n, 2)

        def move(slot, dst, load, src):
            for off, cnt in ((0, SUB), (SUB, 4)):
                for comp, adj, ri in comps:
                    g[par, c, slot * MATS + comp, pl.ds(dst + off, cnt), :] = sign[ri] * load(adj, pl.ds(src + off, cnt))

        def v_local(q, carry):
            move(TB1, XH * q + XH, lambda k, rows: g[flip(par), c, k, rows, :], XH * q)
            return carry
        lax.fori_loop(0, 5, v_local, 0)
        move(TB1, 0, lambda k, rows: tv_in[par, c, k, rows, :], 4)

        def w_all(q, carry):
            move(TB3, XH * q + STRIDE, lambda k, rows: g[flip(par), c, MATS + k, rows, :], XH * q)
            move(TB3, XH * q, lambda k, rows: tw_in[par, c, k, rows, :], XH * q + 4)
            return carry
        lax.fori_loop(0, 3, w_all, 0)
        return carry
    lax.fori_loop(0, 4, t_back, 0)

    for par in (1, 0):
        lz_copy(par).wait_send()
        lz_copy(par).wait_recv()

    def z_back(n, carry):
        par, c = half_of(n), mod(n, 2)

        def body(i, carry):
            rows = rows8(i)
            for typ, k in ((0, NEAR), (1, FAR)):
                packs = [zl_in[par, c, typ, third, rows, :] for third in range(3)]
                back = []
                near_edge = zlane < k
                for comp, adj, ri in comps:
                    own = pltpu.roll(mat(flip(par), c, 4 + typ, adj, rows), k, 1)
                    far = pltpu.roll(packs[adj // COLS], (k + HALF - SUB * (adj % COLS)) % LANES, 1)
                    back.append(sign[ri] * lax.select(near_edge, far, own))
                for comp, val in enumerate(back):
                    g[par, c, (COLS + typ) * MATS + comp, rows, :] = val
            return carry
        lax.fori_loop(0, NV, body, 0)
        return carry
    lax.fori_loop(0, 4, z_back, 0)


    rho0 = red_finish(1)
    scal[0] = rho0
    scal[1] = rho0
    scal[2] = zero

    def cg_step(step, carry):
        def odd_group(c, acc):
            wait_edges(0, c)
            hop(1, c)

            @pl.when(step > 0)
            def _():
                wait_send(1, c)
            wait_far(0, c)

            if c == 0:
                @pl.when(step > 0)
                def _():
                    rho = red_finish(1)
                    norm_ref[pl.ds(step - 1, 1), :] = (rho / scal[0])[0:1]
                    scal[2] = rho / scal[1]
                    scal[1] = rho
            beta = scal[2]

            def body(n, acc):
                packs = []
                for u in range(3):
                    i = n * 3 + u
                    rows, ext = rows8(i), rows8(i + 5)
                    vals = hop_far(1, c, i)
                    for k in range(COLS):
                        s_new = vals[k] + beta * fx[1, c, k, ext, :]
                        p_new = fx[0, c, k, ext, :] + beta * pv[c, k, rows, :]
                        fx[1, c, k, ext, :] = s_new
                        pv[c, k, rows, :] = p_new
                        acc = acc + (s_new * s_new + mass_sq * (p_new * p_new))
                        vals[k] = s_new
                    packs.append((rows, zpack_of(vals)))
                    if c == 1:
                        sums_out(1, i, vals)
                for rows, pack in packs:
                    zs[1, c, rows, :] = pack
                return acc
            acc = lax.fori_loop(0, 3, body, acc)

            if c == 1:
                red_start(0, acc)
            start_halo(1, c)
            return acc
        odd_group(1, odd_group(0, zero))

        def even_group(c, acc):
            wait_edges(1, c)
            hop(0, c)
            wait_send(0, c)
            wait_far(1, c)

            if c == 1:
                scal[3] = scal[1] / red_finish(0)
            alpha = scal[3]

            def body(n, acc):
                packs = []
                for u in range(3):
                    i = n * 3 + u
                    rows, ext = rows8(i), rows8(i + 5)
                    vals = hop_far(0, c, i)
                    for k in range(COLS):
                        p_val = pv[c, k, rows, :]
                        q_val = mass_sq * p_val - vals[k]
                        xv[c, k, rows, :] = xv[c, k, rows, :] + alpha * p_val
                        r_new = fx[0, c, k, ext, :] - alpha * q_val
                        fx[0, c, k, ext, :] = r_new
                        acc = acc + r_new * r_new
                        vals[k] = r_new
                    packs.append((rows, zpack_of(vals)))
                    if c == 1:
                        sums_out(0, i, vals)
                for rows, pack in packs:
                    zs[0, c, rows, :] = pack
                return acc
            acc = lax.fori_loop(0, 3, body, acc)

            if c == 0:
                red_start(1, acc)

            @pl.when(step < ITERS - 1)
            def _():
                start_halo(0, c)
            return acc
        even_group(0, even_group(1, zero))
        return carry
    lax.fori_loop(0, ITERS, cg_step, 0)

    for c in range(2):
        wait_send(1, c)

    def join_sol(blk, carry):
        t, yp = half_of(blk), mod(blk, 2)
        c = yp
        for k in range(COLS):
            dn[0, pl.ds(k, SUB, stride=COLS), :] = xv[c, k, pl.ds(t * XH, SUB), :]
            dn[0, pl.ds(k + 48, 4, stride=COLS), :] = xv[c, k, pl.ds(t * XH + SUB, 4), :]
        for i in range(9):
            val = dn[0, SUB * i:SUB * i + SUB, :]
            sol_ref[t, yp, SUB * i:SUB * i + SUB, :] = val[:, :HALF]
            sol_ref[t, yp + 2, SUB * i:SUB * i + SUB, :] = pltpu.roll(val, HALF, 1)[:, :HALF]
        return carry
    lax.fori_loop(0, XH, join_sol, 0)
    rho = red_finish(1)
    norm_ref[pl.ds(ITERS - 1, 1), :] = (rho / scal[0])[0:1]


def solution(mesh):
    link_spec = P(None, *CUTS)
    field_spec = P(*CUTS)
    vmem = pl.BlockSpec(memory_space=pltpu.VMEM)

    def local_solve(fat_links, long_links, source, quark_mass):
        t_len, z_len, y_len, xh_len = source.shape[:4]

        def link_rows(links):
            return jnp.moveaxis(links, 2, -1).reshape(4, t_len, y_len, STRIDE * xh_len, z_len)
        src = jnp.moveaxis(source, 1, -1).reshape(t_len, y_len, COLS * xh_len, z_len)
        hbm = pl.BlockSpec(memory_space=pl.ANY)
        dma = pltpu.SemaphoreType.DMA
        sol, norms = pl.pallas_call(
            cg_kernel,
            out_shape=(jax.ShapeDtypeStruct(src.shape, F32), jax.ShapeDtypeStruct((SUB, LANES), F32)),
            in_specs=[vmem, pl.BlockSpec(memory_space=pltpu.SMEM), hbm, hbm],
            out_specs=(vmem, vmem),
            scratch_shapes=[
                pltpu.VMEM(PP + (288, ROWS, LANES), F32),
                pltpu.VMEM(PP + (COLS, EXT, LANES), F32),
                pltpu.VMEM(PP + (COLS, ROWS, LANES), F32),
                pltpu.VMEM(PP + (ROWS, LANES), F32),
                pltpu.VMEM(PP + (ROWS, LANES), F32),
                pltpu.VMEM((2, COLS, ROWS, LANES), F32),
                pltpu.VMEM((2, COLS, ROWS, LANES), F32),
                pltpu.VMEM((COLS, ROWS, LANES), F32),
                pltpu.VMEM((ROWS, LANES), jnp.int32),
                pltpu.VMEM((ROWS, LANES), jnp.int32),
                pltpu.VMEM((2, SUB, LANES), F32),
                pltpu.VMEM((2, 16, SUB, LANES), F32),
                pltpu.VMEM((4, SUB, LANES), F32),
                pltpu.VMEM((SLOTS, 2, 2, STRIDE * xh_len, z_len), F32),
                pltpu.VMEM((2, 504, LANES), F32),
                pltpu.VMEM((2, COLS, ROWS, LANES), F32),
                pltpu.VMEM((MATS, ROWS, LANES), F32),
                pltpu.VMEM((MATS, ROWS, LANES), F32),
                pltpu.VMEM(PP + (MATS, 16, LANES), F32),
                pltpu.VMEM(PP + (MATS, BASE, LANES), F32),
                pltpu.VMEM(PP + (2, 3, ROWS, LANES), F32),
                pltpu.VMEM(PP + (2, 3, ROWS, LANES), F32),
                *[dma(n) for n in ((SLOTS, 2, 2), (1,), (1,), PP + (2,), PP + (2,))], dma((2,)), dma((2,)),
                dma(PP + (4,)), dma(PP + (4,)), dma((2, DEVS)), dma((2, DEVS)),
            ],
            compiler_params=pltpu.CompilerParams(has_side_effects=True, vmem_limit_bytes=61 * 1024 * 1024),
        )(src, quark_mass, link_rows(fat_links), link_rows(long_links))
        sol = jnp.moveaxis(sol.reshape(t_len, y_len, xh_len, 3, 2, z_len), -1, 1)
        return sol, norms[:, 0]

    return jax.shard_map(local_solve, mesh=mesh, in_specs=(link_spec, link_spec, field_spec, P()), out_specs=(field_spec, P()), check_vma=False)
```

```python
import jax
import jax.numpy as jnp
from jax import lax
from jax.experimental import pallas as pl
from jax.experimental.pallas import tpu as pltpu
from jax.sharding import PartitionSpec as P

MESH = pl.DeviceIdType.MESH
ITERS = 8
ROWS = 72
NV = 9
EXT = 152
F32 = jnp.float32


SUB, LANES, HALF = 8, 128, 64
BASE = 40
MATS = 18
XH = 12
STRIDE = 36
DEVS = 16
NEAR, FAR = 1, 3
SLOTS = 4
PP = (2, 2)
CUTS = ('t', 'zz', 'yy')
COLS = 6


TF1, TF3, TB1, TB3, ZF1, ZF3, ZB1, ZB3, LS, LO, RS, RO, X0, XP, XM, X2 = range(16)


def flip(bit):
    return 1 - bit


def out_slot_of(mu, typ, yp):
    return {0: TF1 + typ, 1: ZF1 + typ, 2: (LS + (RO - LS) * yp, RO - yp)[typ]}[mu]


def blk_t(blk):
    return blk // 2 if isinstance(blk, int) else half_of(blk)


def blk_y(blk):
    return blk % 2 if isinstance(blk, int) else mod(blk, 2)


def mod(a, n):
    return lax.rem(a, jnp.full_like(a, n))


def half_of(a):
    return lax.div(a, jnp.full_like(a, 2))


def rows8(i):
    return pl.ds(pl.multiple_of(i * SUB, SUB), SUB)


def swap_halves(v):
    return pltpu.roll(v, LANES // 2, 1)


def cg_kernel(src_ref, mass_ref, fat_ref, long_ref, sol_ref, norm_ref,
              g, fx, fy, zs, zr, pv, xv, wv, xh_i, pz_i, red_own, red, scal,
              st, dn, pw, y_out, y_in, tv_in, tw_in, zl_out, zl_in,
              st_sem, ly_send, ly_recv, lt_send, lt_recv, lz_send, lz_recv,
              send_sem, recv_sem, rsend_sem, rrecv_sem):
    yy = lax.axis_index('yy')
    zz = lax.axis_index('zz')
    tt = lax.axis_index('t')
    t_prev, t_next = mod(tt + 3, 4), mod(tt + 1, 4)
    me = yy * SUB + zz * 4 + tt

    raw = (fat_ref, long_ref)

    def raw_copies(mu, blk, slot):
        return [pltpu.make_async_copy(raw[typ].at[mu, blk_t(blk), blk_y(blk) + 2 * h], st.at[slot, typ, h], st_sem.at[slot, typ, h]) for typ in range(2) for h in range(2)]

    MUS = (2, 0, 1, 3)
    for ahead in range(SLOTS - 1):
        for cp in raw_copies(MUS[0], ahead, ahead):
            cp.start()

    lane = lax.broadcasted_iota(jnp.int32, (SUB, LANES), 1)
    sub = lax.broadcasted_iota(jnp.int32, (SUB, LANES), 0)
    zlane = lane % HALF
    zslot = ((lane + 3) % HALF) // SUB
    half1 = lane >= HALF

    def masks(i, carry):
        row = sub + i * SUB
        t_row = row // XH
        xh_i[rows8(i), :] = row - t_row * XH
        pz_i[rows8(i), :] = (t_row + zlane) % 2
        return carry
    lax.fori_loop(0, NV, masks, 0)

    def halo_copies(fi, c, kinds=range(4)):
        def mk(src, dst, kind, dev):
            return pltpu.make_async_remote_copy(src_ref=src, dst_ref=dst, send_sem=send_sem.at[fi, c, kind], recv_sem=recv_sem.at[fi, c, kind], device_id=dev, device_id_type=MESH)
        makers = (
            lambda: mk((fx.at[fi, 0, :, pl.ds(BASE, ROWS), :], pw.at[fi])[c], fy.at[fi, flip(c)], 0, (flip(yy), zz, tt)),
            lambda: mk(fx.at[fi, c, :, pl.ds(BASE, BASE), :], fx.at[fi, c, :, pl.ds(BASE + ROWS, BASE), :], 1, (yy, zz, t_prev)),
            lambda: mk(fx.at[fi, c, :, pl.ds(ROWS, BASE), :], fx.at[fi, c, :, pl.ds(0, BASE), :], 2, (yy, zz, t_next)),
            lambda: mk(zs.at[fi, c], zr.at[fi, c], 3, (yy, flip(zz), tt)),
        )
        return [makers[k]() for k in kinds]

    def start_halo(fi, c, kinds=range(4)):
        for cp in halo_copies(fi, c, kinds):
            cp.start()

    def wait_send(fi, c):
        for cp in halo_copies(fi, c):
            cp.wait_send()

    def wait_edges(fi, c):
        for cp in halo_copies(fi, c, (1, 2, 3)):
            cp.wait_recv()

    def wait_far(fi, c):
        halo_copies(fi, flip(c), (0,))[0].wait_recv()

    peers = []
    for d in range(1, DEVS):
        dev_y = flip(yy) if d // SUB else yy
        dev_z = flip(zz) if (d // 4) % 2 else zz
        dev_t = mod(tt + d % 4, 4)
        peers.append(((dev_y, dev_z, dev_t), dev_y * SUB + dev_z * 4 + mod(tt + 4 - d % 4, 4)))

    def red_copy(slot, d, src_dev):
        return pltpu.make_async_remote_copy(src_ref=red_own.at[slot], dst_ref=red.at[slot, src_dev], send_sem=rsend_sem.at[slot, d], recv_sem=rrecv_sem.at[slot, d], device_id=peers[d - 1][0], device_id_type=MESH)

    def red_start(slot, acc):
        red_own[slot] = acc
        for d in range(1, 16):
            red_copy(slot, d, me).start()

    def red_finish(slot):
        for d in range(1, 16):
            cp = red_copy(slot, d, peers[d - 1][1])
            cp.wait_send()
            cp.wait_recv()
        red[slot, me] = red_own[slot]
        total = red[slot, 0]
        for d in range(1, 16):
            total = total + red[slot, d]
        total = jnp.sum(jnp.sum(total, axis=0, keepdims=True), axis=1, keepdims=True)
        return jnp.broadcast_to(total, (SUB, LANES))

    def mat(par, c, slot, comp, rows):
        return g[par, c, slot * MATS + comp, rows, :]

    def adder(par, c, row, acc):
        def term(slot, vec):
            rows = pl.ds(row, SUB)
            for a in range(3):
                for b in range(3):
                    l_re = mat(par, c, slot, a * COLS + 2 * b, rows)
                    l_im = mat(par, c, slot, a * COLS + 2 * b + 1, rows)
                    v_re, v_im = vec[2 * b], vec[2 * b + 1]
                    for k, t in ((2 * a, l_re * v_re - l_im * v_im), (2 * a + 1, l_re * v_im + l_im * v_re)):
                        acc[k] = t if acc[k] is None else acc[k] + t
        return term

    def hop_own(par, c, i):
        fi = flip(par)
        row = pl.multiple_of(i * SUB, SUB)
        acc = [None] * COLS
        term = adder(par, c, row, acc)

        def ext(off):
            start = row + (BASE + off)
            return [fx[fi, c, k, pl.ds(start, SUB), :] for k in range(COLS)]

        own = ext(0)
        xh = xh_i[pl.ds(row, SUB), :]
        x_even = mod(pz_i[pl.ds(row, SUB), :] + c, 2) == par
        term(X0, own)
        lo, hi = ext(1), ext(-11)
        edge = xh == 11
        term(XP, [lax.select(edge, h, l) for l, h in zip(lo, hi)])
        lo, hi = ext(-1), ext(11)
        edge = xh == 0
        term(XM, [lax.select(edge, h, l) for l, h in zip(lo, hi)])
        m2, m2w, p2, p2w = ext(-2), ext(10), ext(2), ext(-10)
        low, high = xh < 2, xh > 9
        term(X2, [lax.select(x_even, lax.select(low, bw, bm), lax.select(high, fw, fp)) for bm, bw, fp, fw in zip(m2, m2w, p2, p2w)])
        mid = row + BASE
        loc = [fx[fi, flip(c), k, pl.ds(mid, SUB), :] for k in range(COLS)]
        term(LS, loc)
        term(LO, [pltpu.roll(v, HALF, 1) for v in loc])
        zpack = zr[fi, c, pl.ds(row, SUB), :]
        for slot, k in ((ZF1, NEAR), (ZF3, FAR)):
            edge = zlane >= HALF - k
            term(slot, [lax.select(edge, pltpu.roll(zpack, (HALF - k - SUB * j) % LANES, 1), pltpu.roll(own[j], LANES - k, 1)) for j in range(COLS)])
        for slot, k in ((ZB1, NEAR), (ZB3, FAR)):
            edge = zlane < k
            term(slot, [lax.select(edge, pltpu.roll(zpack, (k + HALF - SUB * j) % LANES, 1), pltpu.roll(own[j], k, 1)) for j in range(COLS)])
        term(TF1, ext(XH))
        term(TF3, ext(FAR * XH))
        term(TB1, ext(-XH))
        term(TB3, ext(-FAR * XH))
        return acc

    def hop(par, c):
        def body(i, carry):
            out = hop_own(par, c, i)
            for k in range(COLS):
                wv[k, rows8(i), :] = out[k]
            return carry
        lax.fori_loop(0, NV, body, 0)

    def across(par, c, i, vec, acc):
        term = adder(par, c, pl.multiple_of(i * SUB, SUB), acc)
        term(RS, vec)
        term(RO, [swap_halves(v) for v in vec])
        return acc

    def hop_far(par, c, i):
        rows = rows8(i)
        acc = [wv[k, rows, :] for k in range(COLS)]
        rem = [fy[flip(par), c, k, rows, :] for k in range(COLS)]
        if c == 0:
            return [a + v for a, v in zip(acc, rem)]
        return across(par, c, i, rem, acc)

    def sums_out(fi, i, vals):
        for k, v in enumerate(across(flip(fi), 0, i, vals, [None] * COLS)):
            pw[fi, k, rows8(i), :] = v

    in_slot = [zslot == j for j in range(COLS)]

    def zpack_of(vals):
        packed = vals[0]
        for j in range(1, COLS):
            packed = lax.select(in_slot[j], pltpu.roll(vals[j], SUB * j, 1), packed)
        return packed

    mass = jnp.full((SUB, LANES), mass_ref[0], F32)
    mass_sq = mass * mass
    zero = jnp.zeros((SUB, LANES), F32)

    def split_src(blk, carry):
        t, yp = half_of(blk), mod(blk, 2)
        c = yp
        for i in range(9):
            dn[0, SUB * i:SUB * i + SUB, :] = jnp.concatenate([src_ref[t, yp, SUB * i:SUB * i + SUB, :], src_ref[t, yp + 2, SUB * i:SUB * i + SUB, :]], axis=1)
        for k in range(COLS):
            fx[0, c, k, pl.ds(t * XH + BASE, SUB), :] = dn[0, pl.ds(k, SUB, stride=COLS), :]
            fx[0, c, k, pl.ds(t * XH + 48, 4), :] = dn[0, pl.ds(k + 48, 4, stride=COLS), :]
        return carry
    lax.fori_loop(0, XH, split_src, 0)

    acc = zero
    for c in range(2):
        def init_body(i, acc):
            rows, ext = rows8(i), rows8(i + 5)
            vals = [fx[0, c, k, ext, :] for k in range(COLS)]
            for k in range(COLS):
                fx[1, c, k, ext, :] = zero
                pv[c, k, rows, :] = zero
                xv[c, k, rows, :] = zero
                acc = acc + vals[k] * vals[k]
            zs[0, c, rows, :] = zpack_of(vals)
            return acc
        acc = lax.fori_loop(0, NV, init_body, acc)
        start_halo(0, c, range(c, 4))
    red_start(1, acc)

    c0, c1 = 0, 1
    sign = (-1.0, 1.0)
    comps = [(a * COLS + b * 2 + ri, b * COLS + a * 2 + ri, ri) for a in range(3) for b in range(3) for ri in range(2)]

    def densify(slot, wrap):
        def body(i, carry):
            for u in range(27):
                row = pl.multiple_of(i * (27 * SUB) + u * SUB, SUB)
                for typ in range(2):
                    dn[typ, pl.ds(row + ROWS, SUB), :] = jnp.concatenate([st[slot, typ, 0, pl.ds(row, SUB), :], st[slot, typ, 1, pl.ds(row, SUB), :]], axis=1)
            return carry
        lax.fori_loop(0, 2, body, 0)
        if wrap:
            for typ in range(2):
                dn[typ, :ROWS, :] = dn[typ, COLS * ROWS:, :]

    def base_of(slot):
        return slot * MATS

    def compact(order):
        mu = MUS[order]

        def block(blk, carry):
            slot = mod(blk, SLOTS)
            t, yp = half_of(blk), mod(blk, 2)
            c = yp
            ahead = blk + SLOTS - 1
            ahead_slot = mod(ahead, SLOTS)

            @pl.when(ahead < XH)
            def _():
                for cp in raw_copies(mu, ahead, ahead_slot):
                    cp.start()
            if order < 3:
                @pl.when(ahead >= XH)
                def _():
                    for cp in raw_copies(MUS[order + 1], ahead - XH, ahead_slot):
                        cp.start()
            for cp in raw_copies(mu, blk, slot):
                cp.wait()
            densify(slot, mu == 3)
            for off, n in ((0, SUB), (SUB, 4)):
                out_rows = pl.ds(t * XH + off, n)
                even = mod(zlane[:n] + (t + yp), 2) == 0

                def piece(typ, xpar, comp, back=0):
                    return dn[typ, pl.ds(ROWS + xpar * MATS + comp + STRIDE * (off - back), n, stride=STRIDE), :]

                def put(out_slot, comp, par, val):
                    g[par, c, base_of(out_slot) + comp, out_rows, :] = val
                for comp, adj, ri in comps:
                    if mu != 3:
                        for typ in range(2):
                            out_slot = out_slot_of(mu, typ, yp)
                            e, o = piece(typ, 0, comp), piece(typ, 1, comp)
                            put(out_slot, comp, 0, lax.select(even, e, o))
                            put(out_slot, comp, 1, lax.select(even, o, e))
                    else:
                        pairs = (
                            (X0, piece(0, 0, comp), sign[ri] * piece(0, 0, adj)),
                            (XP, piece(1, 0, comp), piece(0, 1, comp)),
                            (XM, sign[ri] * piece(0, 1, adj, 1), sign[ri] * piece(1, 0, adj, 1)),
                            (X2, sign[ri] * piece(1, 1, adj, 2), piece(1, 1, comp)),
                        )
                        for out_slot, e, o in pairs:
                            put(out_slot, comp, 0, lax.select(even, e, o))
                            put(out_slot, comp, 1, lax.select(even, o, e))
            return carry
        lax.fori_loop(0, XH, block, 0)

    def ly_copy():
        return pltpu.make_async_remote_copy(src_ref=y_out, dst_ref=y_in, send_sem=ly_send.at[0], recv_sem=ly_recv.at[0], device_id=(flip(yy), zz, tt), device_id_type=MESH)

    def lt_copies(par):
        dev = (yy, zz, t_next)
        out = []
        for c in range(2):
            out.append(pltpu.make_async_remote_copy(src_ref=g.at[flip(par), c, pl.ds(0, MATS), pl.ds(56, 16), :], dst_ref=tv_in.at[par, c], send_sem=lt_send.at[par, c, 0], recv_sem=lt_recv.at[par, c, 0], device_id=dev, device_id_type=MESH))
            out.append(pltpu.make_async_remote_copy(src_ref=g.at[flip(par), c, pl.ds(MATS, MATS), pl.ds(32, BASE), :], dst_ref=tw_in.at[par, c], send_sem=lt_send.at[par, c, 1], recv_sem=lt_recv.at[par, c, 1], device_id=dev, device_id_type=MESH))
        return out

    def lz_copy(par):
        return pltpu.make_async_remote_copy(src_ref=zl_out.at[par], dst_ref=zl_in.at[par], send_sem=lz_send.at[par], recv_sem=lz_recv.at[par], device_id=(yy, flip(zz), tt), device_id_type=MESH)

    compact(0)

    def y_pack(i, carry):
        rows = rows8(i)
        w0 = [swap_halves(mat(0, c0, RO, comp, rows)) for comp in range(MATS)]
        for comp in range(MATS):
            y_out[comp, rows, :] = lax.select(half1, mat(1, c0, RO, comp, rows), w0[comp])
        return carry
    lax.fori_loop(0, NV, y_pack, 0)
    ly_copy().start()

    compact(1)
    for par in (1, 0):
        for cp in lt_copies(par):
            cp.start()

    compact(2)

    def z_pack(n, carry):
        par, c = half_of(n), mod(n, 2)

        def body(i, carry):
            rows = rows8(i)
            for typ in range(2):
                for third in range(3):
                    zl_out[par, c, typ, third, rows, :] = zpack_of([mat(flip(par), c, ZF1 + typ, third * COLS + j, rows) for j in range(COLS)])
            return carry
        lax.fori_loop(0, NV, body, 0)
        return carry
    lax.fori_loop(0, 4, z_pack, 0)
    for par in (1, 0):
        lz_copy(par).start()

    def y_local(par, carry):
        def body(i, carry):
            rows = rows8(i)
            for src_c, own_c in ((c1, c0), (c0, c1)):
                far = [swap_halves(mat(flip(par), src_c, RO, adj, rows)) for comp, adj, ri in comps]
                own = [mat(par, own_c, RO, comp, rows) for comp in range(MATS)]
                for comp, adj, ri in comps:
                    g[par, own_c, LO * MATS + comp, rows, :] = lax.select(half1, sign[ri] * far[comp], own[comp])
            v0 = [mat(flip(par), c0, LS, adj, rows) for comp, adj, ri in comps]
            for comp, adj, ri in comps:
                g[par, c1, LS * MATS + comp, rows, :] = sign[ri] * v0[comp]
            return carry
        lax.fori_loop(0, NV, body, 0)
        return carry
    lax.fori_loop(0, 2, y_local, 0)

    def y_far(par):
        def body(i, carry):
            rows = rows8(i)
            w_in = [y_in[comp, rows, :] for comp in range(MATS)]
            if par == 0:
                w_in = [swap_halves(v) for v in w_in]
            v1 = [swap_halves(mat(flip(par), c1, RO, adj, rows)) for comp, adj, ri in comps]
            own = [mat(par, c1, RO, comp, rows) for comp in range(MATS)]
            for comp, adj, ri in comps:
                g[par, c1, RO * MATS + comp, rows, :] = lax.select(half1, own[comp], sign[ri] * w_in[adj])
                g[par, c0, RO * MATS + comp, rows, :] = lax.select(half1, w_in[comp], sign[ri] * v1[comp])
            w1 = [mat(flip(par), c1, RS, adj, rows) for comp, adj, ri in comps]
            for comp, adj, ri in comps:
                g[par, c0, RS * MATS + comp, rows, :] = sign[ri] * w1[comp]
            return carry
        lax.fori_loop(0, NV, body, 0)

    ly_copy().wait_send()
    ly_copy().wait_recv()
    y_far(1)

    def src_sums(i, carry):
        sums_out(0, i, [fx[0, 1, k, rows8(i + 5), :] for k in range(COLS)])
        return carry
    lax.fori_loop(0, NV, src_sums, 0)
    start_halo(0, 1, (0,))
    y_far(0)

    compact(3)

    def derive(par):
        for cp in lt_copies(par) + [lz_copy(par)]:
            cp.wait_send()
            cp.wait_recv()

        def t_back(c, carry):

            def move(slot, dst, load, src):
                for off, cnt in ((0, SUB), (SUB, 4)):
                    for comp, adj, ri in comps:
                        g[par, c, slot * MATS + comp, pl.ds(dst + off, cnt), :] = sign[ri] * load(adj, pl.ds(src + off, cnt))

            def v_local(q, carry):
                move(TB1, XH * q + XH, lambda k, rows: g[flip(par), c, k, rows, :], XH * q)
                return carry
            lax.fori_loop(0, 5, v_local, 0)
            move(TB1, 0, lambda k, rows: tv_in[par, c, k, rows, :], 4)

            def w_all(q, carry):
                move(TB3, XH * q + STRIDE, lambda k, rows: g[flip(par), c, MATS + k, rows, :], XH * q)
                move(TB3, XH * q, lambda k, rows: tw_in[par, c, k, rows, :], XH * q + 4)
                return carry
            lax.fori_loop(0, 3, w_all, 0)
            return carry
        lax.fori_loop(0, 2, t_back, 0)

        def z_back(c, carry):

            def body(i, carry):
                rows = rows8(i)
                for typ, k in ((0, NEAR), (1, FAR)):
                    packs = [zl_in[par, c, typ, third, rows, :] for third in range(3)]
                    back = []
                    near_edge = zlane < k
                    for comp, adj, ri in comps:
                        own = pltpu.roll(mat(flip(par), c, 4 + typ, adj, rows), k, 1)
                        far = pltpu.roll(packs[adj // COLS], (k + HALF - SUB * (adj % COLS)) % LANES, 1)
                        back.append(sign[ri] * lax.select(near_edge, far, own))
                    for comp, val in enumerate(back):
                        g[par, c, (COLS + typ) * MATS + comp, rows, :] = val
                return carry
            lax.fori_loop(0, NV, body, 0)
            return carry
        lax.fori_loop(0, 2, z_back, 0)

    derive(1)
    rho0 = red_finish(1)
    scal[0] = rho0
    scal[1] = rho0
    scal[2] = zero

    def cg_step(step, carry):
        def odd_group(c):
            acc = zero if c == 0 else scal[4]

            @pl.when(step > 0)
            def _():
                wait_send(1, c)
            wait_far(0, c)

            if c == 0:
                @pl.when(step > 0)
                def _():
                    rho = red_finish(1)
                    norm_ref[pl.ds(step - 1, 1), :] = (rho / scal[0])[0:1]
                    scal[2] = rho / scal[1]
                    scal[1] = rho
            beta = scal[2]

            def body(n, acc):
                packs = []
                for u in range(3):
                    i = n * 3 + u
                    rows, ext = rows8(i), rows8(i + 5)
                    vals = hop_far(1, c, i)
                    for k in range(COLS):
                        s_new = vals[k] + beta * fx[1, c, k, ext, :]
                        p_new = fx[0, c, k, ext, :] + beta * pv[c, k, rows, :]
                        fx[1, c, k, ext, :] = s_new
                        pv[c, k, rows, :] = p_new
                        acc = acc + (s_new * s_new + mass_sq * (p_new * p_new))
                        vals[k] = s_new
                    packs.append((rows, zpack_of(vals)))
                    if c == 1:
                        sums_out(1, i, vals)
                for rows, pack in packs:
                    zs[1, c, rows, :] = pack
                return acc
            acc = lax.fori_loop(0, 3, body, acc)

            if c == 1:
                red_start(0, acc)
            else:
                scal[4] = acc
            start_halo(1, c)

        def odd_pass(c, carry):
            wait_edges(0, c)
            hop(1, c)
            pl.when(c == 0)(lambda: odd_group(0))
            pl.when(c == 1)(lambda: odd_group(1))
            return carry
        lax.fori_loop(0, 2, odd_pass, 0)

        @pl.when(step == 0)
        def _():
            derive(0)

        def even_group(c):
            acc = zero if c == 1 else scal[4]
            wait_send(0, c)
            wait_far(1, c)

            if c == 1:
                scal[3] = scal[1] / red_finish(0)
            alpha = scal[3]

            def body(n, acc):
                packs = []
                for u in range(3):
                    i = n * 3 + u
                    rows, ext = rows8(i), rows8(i + 5)
                    vals = hop_far(0, c, i)
                    for k in range(COLS):
                        p_val = pv[c, k, rows, :]
                        q_val = mass_sq * p_val - vals[k]
                        xv[c, k, rows, :] = xv[c, k, rows, :] + alpha * p_val
                        r_new = fx[0, c, k, ext, :] - alpha * q_val
                        fx[0, c, k, ext, :] = r_new
                        acc = acc + r_new * r_new
                        vals[k] = r_new
                    packs.append((rows, zpack_of(vals)))
                    if c == 1:
                        sums_out(0, i, vals)
                for rows, pack in packs:
                    zs[0, c, rows, :] = pack
                return acc
            acc = lax.fori_loop(0, 3, body, acc)

            if c == 0:
                red_start(1, acc)
            else:
                scal[4] = acc

            @pl.when(step < ITERS - 1)
            def _():
                start_halo(0, c)

        def even_pass(n, carry):
            c = flip(n)
            wait_edges(1, c)
            hop(0, c)
            pl.when(c == 1)(lambda: even_group(1))
            pl.when(c == 0)(lambda: even_group(0))
            return carry
        lax.fori_loop(0, 2, even_pass, 0)
        return carry
    lax.fori_loop(0, ITERS, cg_step, 0)

    for c in range(2):
        wait_send(1, c)

    def join_sol(blk, carry):
        t, yp = half_of(blk), mod(blk, 2)
        c = yp
        for k in range(COLS):
            dn[0, pl.ds(k, SUB, stride=COLS), :] = xv[c, k, pl.ds(t * XH, SUB), :]
            dn[0, pl.ds(k + 48, 4, stride=COLS), :] = xv[c, k, pl.ds(t * XH + SUB, 4), :]
        for i in range(9):
            val = dn[0, SUB * i:SUB * i + SUB, :]
            sol_ref[t, yp, SUB * i:SUB * i + SUB, :] = val[:, :HALF]
            sol_ref[t, yp + 2, SUB * i:SUB * i + SUB, :] = pltpu.roll(val, HALF, 1)[:, :HALF]
        return carry
    lax.fori_loop(0, XH, join_sol, 0)
    rho = red_finish(1)
    norm_ref[pl.ds(ITERS - 1, 1), :] = (rho / scal[0])[0:1]


def solution(mesh):
    link_spec = P(None, *CUTS)
    field_spec = P(*CUTS)
    vmem = pl.BlockSpec(memory_space=pltpu.VMEM)

    def local_solve(fat_links, long_links, source, quark_mass):
        t_len, z_len, y_len, xh_len = source.shape[:4]

        def link_rows(links):
            return jnp.moveaxis(links, 2, -1).reshape(4, t_len, y_len, STRIDE * xh_len, z_len)
        src = jnp.moveaxis(source, 1, -1).reshape(t_len, y_len, COLS * xh_len, z_len)
        hbm = pl.BlockSpec(memory_space=pl.ANY)
        dma = pltpu.SemaphoreType.DMA
        sol, norms = pl.pallas_call(
            cg_kernel,
            out_shape=(jax.ShapeDtypeStruct(src.shape, F32), jax.ShapeDtypeStruct((SUB, LANES), F32)),
            in_specs=[vmem, pl.BlockSpec(memory_space=pltpu.SMEM), hbm, hbm],
            out_specs=(vmem, vmem),
            scratch_shapes=[
                pltpu.VMEM(PP + (288, ROWS, LANES), F32),
                pltpu.VMEM(PP + (COLS, EXT, LANES), F32),
                pltpu.VMEM(PP + (COLS, ROWS, LANES), F32),
                pltpu.VMEM(PP + (ROWS, LANES), F32),
                pltpu.VMEM(PP + (ROWS, LANES), F32),
                pltpu.VMEM((2, COLS, ROWS, LANES), F32),
                pltpu.VMEM((2, COLS, ROWS, LANES), F32),
                pltpu.VMEM((COLS, ROWS, LANES), F32),
                pltpu.VMEM((ROWS, LANES), jnp.int32),
                pltpu.VMEM((ROWS, LANES), jnp.int32),
                pltpu.VMEM((2, SUB, LANES), F32),
                pltpu.VMEM((2, 16, SUB, LANES), F32),
                pltpu.VMEM((5, SUB, LANES), F32),
                pltpu.VMEM((SLOTS, 2, 2, STRIDE * xh_len, z_len), F32),
                pltpu.VMEM((2, 504, LANES), F32),
                pltpu.VMEM((2, COLS, ROWS, LANES), F32),
                pltpu.VMEM((MATS, ROWS, LANES), F32),
                pltpu.VMEM((MATS, ROWS, LANES), F32),
                pltpu.VMEM(PP + (MATS, 16, LANES), F32),
                pltpu.VMEM(PP + (MATS, BASE, LANES), F32),
                pltpu.VMEM(PP + (2, 3, ROWS, LANES), F32),
                pltpu.VMEM(PP + (2, 3, ROWS, LANES), F32),
                *[dma(n) for n in ((SLOTS, 2, 2), (1,), (1,), PP + (2,), PP + (2,))], dma((2,)), dma((2,)),
                dma(PP + (4,)), dma(PP + (4,)), dma((2, DEVS)), dma((2, DEVS)),
            ],
            compiler_params=pltpu.CompilerParams(has_side_effects=True, vmem_limit_bytes=61 * 1024 * 1024),
        )(src, quark_mass, link_rows(fat_links), link_rows(long_links))
        sol = jnp.moveaxis(sol.reshape(t_len, y_len, xh_len, 3, 2, z_len), -1, 1)
        return sol, norms[:, 0]

    return jax.shard_map(local_solve, mesh=mesh, in_specs=(link_spec, link_spec, field_spec, P()), out_specs=(field_spec, P()), check_vma=False)
```

```python
import jax
import jax.numpy as jnp
from jax import lax
from jax.experimental import pallas as pl
from jax.experimental.pallas import tpu as pltpu
from jax.sharding import PartitionSpec as P

MESH = pl.DeviceIdType.MESH
ITERS = 8
ROWS = 72
NV = 9
EXT = 152
F32 = jnp.float32


SUB, LANES, HALF = 8, 128, 64
BASE = 40
MATS = 18
XH = 12
STRIDE = 36
DEVS = 16
NEAR, FAR = 1, 3
SLOTS = 6
PP = (2, 2)
CUTS = ('t', 'zz', 'yy')
COLS = 6


TF1, TF3, TB1, TB3, ZF1, ZF3, ZB1, ZB3, LS, LO, RS, RO, X0, XP, XM, X2 = range(16)


def flip(bit):
    return 1 - bit


def out_slot_of(mu, typ, yp):
    return {0: TF1 + typ, 1: ZF1 + typ, 2: (LS + (RO - LS) * yp, RO - yp)[typ]}[mu]


def blk_t(blk):
    return blk // 2 if isinstance(blk, int) else half_of(blk)


def blk_y(blk):
    return blk % 2 if isinstance(blk, int) else mod(blk, 2)


def mod(a, n):
    return lax.rem(a, jnp.full_like(a, n))


def half_of(a):
    return lax.div(a, jnp.full_like(a, 2))


def rows8(i):
    return pl.ds(pl.multiple_of(i * SUB, SUB), SUB)


def swap_halves(v):
    return pltpu.roll(v, LANES // 2, 1)


def cg_kernel(src_ref, mass_ref, fat_ref, long_ref, sol_ref, norm_ref,
              g, fx, fy, zs, zr, pv, xv, wv, xh_i, pz_i, red_own, red, scal,
              st, dn, pw, y_out, y_in, tv_in, tw_in, zl_out, zl_in,
              st_sem, ly_send, ly_recv, lt_send, lt_recv, lz_send, lz_recv,
              send_sem, recv_sem, rsend_sem, rrecv_sem):
    yy = lax.axis_index('yy')
    zz = lax.axis_index('zz')
    tt = lax.axis_index('t')
    t_prev, t_next = mod(tt + 3, 4), mod(tt + 1, 4)
    me = yy * SUB + zz * 4 + tt

    raw = (fat_ref, long_ref)

    def raw_copies(mu, blk, slot):
        return [pltpu.make_async_copy(raw[typ].at[mu, blk_t(blk), blk_y(blk) + 2 * h], st.at[slot, typ, h], st_sem.at[slot, typ, h]) for typ in range(2) for h in range(2)]

    MUS = (2, 0, 1, 3)
    for ahead in range(SLOTS - 1):
        for cp in raw_copies(MUS[0], ahead, ahead):
            cp.start()

    lane = lax.broadcasted_iota(jnp.int32, (SUB, LANES), 1)
    sub = lax.broadcasted_iota(jnp.int32, (SUB, LANES), 0)
    zlane = lane % HALF
    zslot = ((lane + 3) % HALF) // SUB
    half1 = lane >= HALF

    def masks(i, carry):
        row = sub + i * SUB
        t_row = row // XH
        xh_i[rows8(i), :] = row - t_row * XH
        pz_i[rows8(i), :] = (t_row + zlane) % 2
        return carry
    lax.fori_loop(0, NV, masks, 0)

    def halo_copies(fi, c, kinds=range(4)):
        def mk(src, dst, kind, dev):
            return pltpu.make_async_remote_copy(src_ref=src, dst_ref=dst, send_sem=send_sem.at[fi, c, kind], recv_sem=recv_sem.at[fi, c, kind], device_id=dev, device_id_type=MESH)
        makers = (
            lambda: mk((fx.at[fi, 0, :, pl.ds(BASE, ROWS), :], pw.at[fi])[c], fy.at[fi, flip(c)], 0, (flip(yy), zz, tt)),
            lambda: mk(fx.at[fi, c, :, pl.ds(BASE, BASE), :], fx.at[fi, c, :, pl.ds(BASE + ROWS, BASE), :], 1, (yy, zz, t_prev)),
            lambda: mk(fx.at[fi, c, :, pl.ds(ROWS, BASE), :], fx.at[fi, c, :, pl.ds(0, BASE), :], 2, (yy, zz, t_next)),
            lambda: mk(zs.at[fi, c], zr.at[fi, c], 3, (yy, flip(zz), tt)),
        )
        return [makers[k]() for k in kinds]

    def start_halo(fi, c, kinds=range(4)):
        for cp in halo_copies(fi, c, kinds):
            cp.start()

    def wait_send(fi, c):
        for cp in halo_copies(fi, c):
            cp.wait_send()

    def wait_edges(fi, c):
        for cp in halo_copies(fi, c, (1, 2, 3)):
            cp.wait_recv()

    def wait_far(fi, c):
        halo_copies(fi, flip(c), (0,))[0].wait_recv()

    peers = []
    for d in range(1, DEVS):
        dev_y = flip(yy) if d // SUB else yy
        dev_z = flip(zz) if (d // 4) % 2 else zz
        dev_t = mod(tt + d % 4, 4)
        peers.append(((dev_y, dev_z, dev_t), dev_y * SUB + dev_z * 4 + mod(tt + 4 - d % 4, 4)))

    def red_copy(slot, d, src_dev):
        return pltpu.make_async_remote_copy(src_ref=red_own.at[slot], dst_ref=red.at[slot, src_dev], send_sem=rsend_sem.at[slot, d], recv_sem=rrecv_sem.at[slot, d], device_id=peers[d - 1][0], device_id_type=MESH)

    def red_start(slot, acc):
        red_own[slot] = acc
        for d in range(1, 16):
            red_copy(slot, d, me).start()

    def red_finish(slot):
        for d in range(1, 16):
            cp = red_copy(slot, d, peers[d - 1][1])
            cp.wait_send()
            cp.wait_recv()
        red[slot, me] = red_own[slot]
        total = red[slot, 0]
        for d in range(1, 16):
            total = total + red[slot, d]
        total = jnp.sum(jnp.sum(total, axis=0, keepdims=True), axis=1, keepdims=True)
        return jnp.broadcast_to(total, (SUB, LANES))

    def mat(par, c, slot, comp, rows):
        return g[par, c, slot * MATS + comp, rows, :]

    def adder(par, c, row, acc):
        def term(slot, vec):
            rows = pl.ds(row, SUB)
            for a in range(3):
                for b in range(3):
                    l_re = mat(par, c, slot, a * COLS + 2 * b, rows)
                    l_im = mat(par, c, slot, a * COLS + 2 * b + 1, rows)
                    v_re, v_im = vec[2 * b], vec[2 * b + 1]
                    for k, t in ((2 * a, l_re * v_re - l_im * v_im), (2 * a + 1, l_re * v_im + l_im * v_re)):
                        acc[k] = t if acc[k] is None else acc[k] + t
        return term

    def hop_own(par, c, i):
        fi = flip(par)
        row = pl.multiple_of(i * SUB, SUB)
        acc = [None] * COLS
        term = adder(par, c, row, acc)

        def ext(off):
            start = row + (BASE + off)
            return [fx[fi, c, k, pl.ds(start, SUB), :] for k in range(COLS)]

        own = ext(0)
        xh = xh_i[pl.ds(row, SUB), :]
        x_even = mod(pz_i[pl.ds(row, SUB), :] + c, 2) == par
        term(X0, own)
        lo, hi = ext(1), ext(-11)
        edge = xh == 11
        term(XP, [lax.select(edge, h, l) for l, h in zip(lo, hi)])
        lo, hi = ext(-1), ext(11)
        edge = xh == 0
        term(XM, [lax.select(edge, h, l) for l, h in zip(lo, hi)])
        m2, m2w, p2, p2w = ext(-2), ext(10), ext(2), ext(-10)
        low, high = xh < 2, xh > 9
        term(X2, [lax.select(x_even, lax.select(low, bw, bm), lax.select(high, fw, fp)) for bm, bw, fp, fw in zip(m2, m2w, p2, p2w)])
        mid = row + BASE
        loc = [fx[fi, flip(c), k, pl.ds(mid, SUB), :] for k in range(COLS)]
        term(LS, loc)
        term(LO, [pltpu.roll(v, HALF, 1) for v in loc])
        zpack = zr[fi, c, pl.ds(row, SUB), :]
        for slot, k in ((ZF1, NEAR), (ZF3, FAR)):
            edge = zlane >= HALF - k
            term(slot, [lax.select(edge, pltpu.roll(zpack, (HALF - k - SUB * j) % LANES, 1), pltpu.roll(own[j], LANES - k, 1)) for j in range(COLS)])
        for slot, k in ((ZB1, NEAR), (ZB3, FAR)):
            edge = zlane < k
            term(slot, [lax.select(edge, pltpu.roll(zpack, (k + HALF - SUB * j) % LANES, 1), pltpu.roll(own[j], k, 1)) for j in range(COLS)])
        term(TF1, ext(XH))
        term(TF3, ext(FAR * XH))
        term(TB1, ext(-XH))
        term(TB3, ext(-FAR * XH))
        return acc

    def hop(par, c):
        def body(i, carry):
            out = hop_own(par, c, i)
            for k in range(COLS):
                wv[k, rows8(i), :] = out[k]
            return carry
        lax.fori_loop(0, NV, body, 0)

    def across(par, c, i, vec, acc):
        term = adder(par, c, pl.multiple_of(i * SUB, SUB), acc)
        term(RS, vec)
        term(RO, [swap_halves(v) for v in vec])
        return acc

    def hop_far(par, c, i):
        rows = rows8(i)
        acc = [wv[k, rows, :] for k in range(COLS)]
        rem = [fy[flip(par), c, k, rows, :] for k in range(COLS)]
        if c == 0:
            return [a + v for a, v in zip(acc, rem)]
        return across(par, c, i, rem, acc)

    def sums_out(fi, i, vals):
        for k, v in enumerate(across(flip(fi), 0, i, vals, [None] * COLS)):
            pw[fi, k, rows8(i), :] = v

    in_slot = [zslot == j for j in range(COLS)]

    def zpack_of(vals):
        packed = vals[0]
        for j in range(1, COLS):
            packed = lax.select(in_slot[j], pltpu.roll(vals[j], SUB * j, 1), packed)
        return packed

    mass = jnp.full((SUB, LANES), mass_ref[0], F32)
    mass_sq = mass * mass
    zero = jnp.zeros((SUB, LANES), F32)

    def split_src(blk, carry):
        t, yp = half_of(blk), mod(blk, 2)
        c = yp
        for i in range(9):
            dn[0, SUB * i:SUB * i + SUB, :] = jnp.concatenate([src_ref[t, yp, SUB * i:SUB * i + SUB, :], src_ref[t, yp + 2, SUB * i:SUB * i + SUB, :]], axis=1)
        for k in range(COLS):
            fx[0, c, k, pl.ds(t * XH + BASE, SUB), :] = dn[0, pl.ds(k, SUB, stride=COLS), :]
            fx[0, c, k, pl.ds(t * XH + 48, 4), :] = dn[0, pl.ds(k + 48, 4, stride=COLS), :]
        return carry
    lax.fori_loop(0, XH, split_src, 0)

    acc = zero
    for c in range(2):
        def init_body(i, acc):
            rows, ext = rows8(i), rows8(i + 5)
            vals = [fx[0, c, k, ext, :] for k in range(COLS)]
            for k in range(COLS):
                fx[1, c, k, ext, :] = zero
                pv[c, k, rows, :] = zero
                xv[c, k, rows, :] = zero
                acc = acc + vals[k] * vals[k]
            zs[0, c, rows, :] = zpack_of(vals)
            return acc
        acc = lax.fori_loop(0, NV, init_body, acc)
        start_halo(0, c, range(c, 4))
    red_start(1, acc)

    c0, c1 = 0, 1
    sign = (-1.0, 1.0)
    comps = [(a * COLS + b * 2 + ri, b * COLS + a * 2 + ri, ri) for a in range(3) for b in range(3) for ri in range(2)]

    def densify(slot, wrap):
        def body(i, carry):
            for u in range(27):
                row = pl.multiple_of(i * (27 * SUB) + u * SUB, SUB)
                for typ in range(2):
                    dn[typ, pl.ds(row + ROWS, SUB), :] = jnp.concatenate([st[slot, typ, 0, pl.ds(row, SUB), :], st[slot, typ, 1, pl.ds(row, SUB), :]], axis=1)
            return carry
        lax.fori_loop(0, 2, body, 0)
        if wrap:
            for typ in range(2):
                dn[typ, :ROWS, :] = dn[typ, COLS * ROWS:, :]

    def base_of(slot):
        return slot * MATS

    def compact(order):
        mu = MUS[order]

        def block(blk, carry):
            slot = mod(blk, SLOTS)
            t, yp = half_of(blk), mod(blk, 2)
            c = yp
            ahead = blk + SLOTS - 1
            ahead_slot = mod(ahead, SLOTS)

            @pl.when(ahead < XH)
            def _():
                for cp in raw_copies(mu, ahead, ahead_slot):
                    cp.start()
            if order < 3:
                @pl.when(ahead >= XH)
                def _():
                    for cp in raw_copies(MUS[order + 1], ahead - XH, ahead_slot):
                        cp.start()
            for cp in raw_copies(mu, blk, slot):
                cp.wait()
            densify(slot, mu == 3)
            for off, n in ((0, SUB), (SUB, 4)):
                out_rows = pl.ds(t * XH + off, n)
                even = mod(zlane[:n] + (t + yp), 2) == 0

                def piece(typ, xpar, comp, back=0):
                    return dn[typ, pl.ds(ROWS + xpar * MATS + comp + STRIDE * (off - back), n, stride=STRIDE), :]

                def put(out_slot, comp, par, val):
                    g[par, c, base_of(out_slot) + comp, out_rows, :] = val
                for comp, adj, ri in comps:
                    if mu != 3:
                        for typ in range(2):
                            out_slot = out_slot_of(mu, typ, yp)
                            e, o = piece(typ, 0, comp), piece(typ, 1, comp)
                            put(out_slot, comp, 0, lax.select(even, e, o))
                            put(out_slot, comp, 1, lax.select(even, o, e))
                    else:
                        pairs = (
                            (X0, piece(0, 0, comp), sign[ri] * piece(0, 0, adj)),
                            (XP, piece(1, 0, comp), piece(0, 1, comp)),
                            (XM, sign[ri] * piece(0, 1, adj, 1), sign[ri] * piece(1, 0, adj, 1)),
                            (X2, sign[ri] * piece(1, 1, adj, 2), piece(1, 1, comp)),
                        )
                        for out_slot, e, o in pairs:
                            put(out_slot, comp, 0, lax.select(even, e, o))
                            put(out_slot, comp, 1, lax.select(even, o, e))
            return carry
        lax.fori_loop(0, XH, block, 0)

    def ly_copy():
        return pltpu.make_async_remote_copy(src_ref=y_out, dst_ref=y_in, send_sem=ly_send.at[0], recv_sem=ly_recv.at[0], device_id=(flip(yy), zz, tt), device_id_type=MESH)

    def lt_copies(par):
        dev = (yy, zz, t_next)
        out = []
        for c in range(2):
            out.append(pltpu.make_async_remote_copy(src_ref=g.at[flip(par), c, pl.ds(0, MATS), pl.ds(56, 16), :], dst_ref=tv_in.at[par, c], send_sem=lt_send.at[par, c, 0], recv_sem=lt_recv.at[par, c, 0], device_id=dev, device_id_type=MESH))
            out.append(pltpu.make_async_remote_copy(src_ref=g.at[flip(par), c, pl.ds(MATS, MATS), pl.ds(32, BASE), :], dst_ref=tw_in.at[par, c], send_sem=lt_send.at[par, c, 1], recv_sem=lt_recv.at[par, c, 1], device_id=dev, device_id_type=MESH))
        return out

    def lz_copy(par):
        return pltpu.make_async_remote_copy(src_ref=zl_out.at[par], dst_ref=zl_in.at[par], send_sem=lz_send.at[par], recv_sem=lz_recv.at[par], device_id=(yy, flip(zz), tt), device_id_type=MESH)

    compact(0)

    def y_pack(i, carry):
        rows = rows8(i)
        w0 = [swap_halves(mat(0, c0, RO, comp, rows)) for comp in range(MATS)]
        for comp in range(MATS):
            y_out[comp, rows, :] = lax.select(half1, mat(1, c0, RO, comp, rows), w0[comp])
        return carry
    lax.fori_loop(0, NV, y_pack, 0)
    ly_copy().start()

    compact(1)
    for par in (1, 0):
        for cp in lt_copies(par):
            cp.start()

    compact(2)

    def z_pack(n, carry):
        par, c = half_of(n), mod(n, 2)

        def body(i, carry):
            rows = rows8(i)
            for typ in range(2):
                for third in range(3):
                    zl_out[par, c, typ, third, rows, :] = zpack_of([mat(flip(par), c, ZF1 + typ, third * COLS + j, rows) for j in range(COLS)])
            return carry
        lax.fori_loop(0, NV, body, 0)
        return carry
    lax.fori_loop(0, 4, z_pack, 0)
    for par in (1, 0):
        lz_copy(par).start()

    def y_local(par, carry):
        def body(i, carry):
            rows = rows8(i)
            for src_c, own_c in ((c1, c0), (c0, c1)):
                far = [swap_halves(mat(flip(par), src_c, RO, adj, rows)) for comp, adj, ri in comps]
                own = [mat(par, own_c, RO, comp, rows) for comp in range(MATS)]
                for comp, adj, ri in comps:
                    g[par, own_c, LO * MATS + comp, rows, :] = lax.select(half1, sign[ri] * far[comp], own[comp])
            v0 = [mat(flip(par), c0, LS, adj, rows) for comp, adj, ri in comps]
            for comp, adj, ri in comps:
                g[par, c1, LS * MATS + comp, rows, :] = sign[ri] * v0[comp]
            return carry
        lax.fori_loop(0, NV, body, 0)
        return carry
    lax.fori_loop(0, 2, y_local, 0)

    def y_far(par):
        def body(i, carry):
            rows = rows8(i)
            w_in = [y_in[comp, rows, :] for comp in range(MATS)]
            if par == 0:
                w_in = [swap_halves(v) for v in w_in]
            v1 = [swap_halves(mat(flip(par), c1, RO, adj, rows)) for comp, adj, ri in comps]
            own = [mat(par, c1, RO, comp, rows) for comp in range(MATS)]
            for comp, adj, ri in comps:
                g[par, c1, RO * MATS + comp, rows, :] = lax.select(half1, own[comp], sign[ri] * w_in[adj])
                g[par, c0, RO * MATS + comp, rows, :] = lax.select(half1, w_in[comp], sign[ri] * v1[comp])
            w1 = [mat(flip(par), c1, RS, adj, rows) for comp, adj, ri in comps]
            for comp, adj, ri in comps:
                g[par, c0, RS * MATS + comp, rows, :] = sign[ri] * w1[comp]
            return carry
        lax.fori_loop(0, NV, body, 0)

    ly_copy().wait_send()
    ly_copy().wait_recv()
    y_far(1)

    def src_sums(i, carry):
        sums_out(0, i, [fx[0, 1, k, rows8(i + 5), :] for k in range(COLS)])
        return carry
    lax.fori_loop(0, NV, src_sums, 0)
    start_halo(0, 1, (0,))
    y_far(0)

    compact(3)

    def derive(par):
        for cp in lt_copies(par) + [lz_copy(par)]:
            cp.wait_send()
            cp.wait_recv()

        def t_back(c, carry):

            def move(slot, dst, load, src):
                for off, cnt in ((0, SUB), (SUB, 4)):
                    for comp, adj, ri in comps:
                        g[par, c, slot * MATS + comp, pl.ds(dst + off, cnt), :] = sign[ri] * load(adj, pl.ds(src + off, cnt))

            def v_local(q, carry):
                move(TB1, XH * q + XH, lambda k, rows: g[flip(par), c, k, rows, :], XH * q)
                return carry
            lax.fori_loop(0, 5, v_local, 0)
            move(TB1, 0, lambda k, rows: tv_in[par, c, k, rows, :], 4)

            def w_all(q, carry):
                move(TB3, XH * q + STRIDE, lambda k, rows: g[flip(par), c, MATS + k, rows, :], XH * q)
                move(TB3, XH * q, lambda k, rows: tw_in[par, c, k, rows, :], XH * q + 4)
                return carry
            lax.fori_loop(0, 3, w_all, 0)
            return carry
        lax.fori_loop(0, 2, t_back, 0)

        def z_back(c, carry):

            def body(i, carry):
                rows = rows8(i)
                for typ, k in ((0, NEAR), (1, FAR)):
                    packs = [zl_in[par, c, typ, third, rows, :] for third in range(3)]
                    back = []
                    near_edge = zlane < k
                    for comp, adj, ri in comps:
                        own = pltpu.roll(mat(flip(par), c, 4 + typ, adj, rows), k, 1)
                        far = pltpu.roll(packs[adj // COLS], (k + HALF - SUB * (adj % COLS)) % LANES, 1)
                        back.append(sign[ri] * lax.select(near_edge, far, own))
                    for comp, val in enumerate(back):
                        g[par, c, (COLS + typ) * MATS + comp, rows, :] = val
                return carry
            lax.fori_loop(0, NV, body, 0)
            return carry
        lax.fori_loop(0, 2, z_back, 0)

    derive(1)
    rho0 = red_finish(1)
    scal[0] = rho0
    scal[1] = rho0
    scal[2] = zero

    def cg_step(step, carry):
        def odd_group(c):
            acc = zero if c == 0 else scal[4]

            @pl.when(step > 0)
            def _():
                wait_send(1, c)
            wait_far(0, c)

            if c == 0:
                @pl.when(step > 0)
                def _():
                    rho = red_finish(1)
                    norm_ref[pl.ds(step - 1, 1), :] = (rho / scal[0])[0:1]
                    scal[2] = rho / scal[1]
                    scal[1] = rho
            beta = scal[2]

            def body(n, acc):
                packs = []
                for u in range(3):
                    i = n * 3 + u
                    rows, ext = rows8(i), rows8(i + 5)
                    vals = hop_far(1, c, i)
                    for k in range(COLS):
                        s_new = vals[k] + beta * fx[1, c, k, ext, :]
                        p_new = fx[0, c, k, ext, :] + beta * pv[c, k, rows, :]
                        fx[1, c, k, ext, :] = s_new
                        pv[c, k, rows, :] = p_new
                        acc = acc + (s_new * s_new + mass_sq * (p_new * p_new))
                        vals[k] = s_new
                    packs.append((rows, zpack_of(vals)))
                    if c == 1:
                        sums_out(1, i, vals)
                for rows, pack in packs:
                    zs[1, c, rows, :] = pack
                return acc
            acc = lax.fori_loop(0, 3, body, acc)

            if c == 1:
                red_start(0, acc)
            else:
                scal[4] = acc
            start_halo(1, c)

        def odd_pass(c, carry):
            wait_edges(0, c)
            hop(1, c)
            pl.when(c == 0)(lambda: odd_group(0))
            pl.when(c == 1)(lambda: odd_group(1))
            return carry
        lax.fori_loop(0, 2, odd_pass, 0)

        @pl.when(step == 0)
        def _():
            derive(0)

        def even_group(c):
            acc = zero if c == 1 else scal[4]
            wait_send(0, c)
            wait_far(1, c)

            if c == 1:
                scal[3] = scal[1] / red_finish(0)
            alpha = scal[3]

            def body(n, acc):
                packs = []
                for u in range(3):
                    i = n * 3 + u
                    rows, ext = rows8(i), rows8(i + 5)
                    vals = hop_far(0, c, i)
                    for k in range(COLS):
                        p_val = pv[c, k, rows, :]
                        q_val = mass_sq * p_val - vals[k]
                        xv[c, k, rows, :] = xv[c, k, rows, :] + alpha * p_val
                        r_new = fx[0, c, k, ext, :] - alpha * q_val
                        fx[0, c, k, ext, :] = r_new
                        acc = acc + r_new * r_new
                        vals[k] = r_new
                    packs.append((rows, zpack_of(vals)))
                    if c == 1:
                        sums_out(0, i, vals)
                for rows, pack in packs:
                    zs[0, c, rows, :] = pack
                return acc
            acc = lax.fori_loop(0, 3, body, acc)

            if c == 0:
                red_start(1, acc)
            else:
                scal[4] = acc

            @pl.when(step < ITERS - 1)
            def _():
                start_halo(0, c)

        def even_pass(n, carry):
            c = flip(n)
            wait_edges(1, c)
            hop(0, c)
            pl.when(c == 1)(lambda: even_group(1))
            pl.when(c == 0)(lambda: even_group(0))
            return carry
        lax.fori_loop(0, 2, even_pass, 0)
        return carry
    lax.fori_loop(0, ITERS, cg_step, 0)

    for c in range(2):
        wait_send(1, c)

    def join_sol(blk, carry):
        t, yp = half_of(blk), mod(blk, 2)
        c = yp
        for k in range(COLS):
            dn[0, pl.ds(k, SUB, stride=COLS), :] = xv[c, k, pl.ds(t * XH, SUB), :]
            dn[0, pl.ds(k + 48, 4, stride=COLS), :] = xv[c, k, pl.ds(t * XH + SUB, 4), :]
        for i in range(9):
            val = dn[0, SUB * i:SUB * i + SUB, :]
            sol_ref[t, yp, SUB * i:SUB * i + SUB, :] = val[:, :HALF]
            sol_ref[t, yp + 2, SUB * i:SUB * i + SUB, :] = pltpu.roll(val, HALF, 1)[:, :HALF]
        return carry
    lax.fori_loop(0, XH, join_sol, 0)
    rho = red_finish(1)
    norm_ref[pl.ds(ITERS - 1, 1), :] = (rho / scal[0])[0:1]


def solution(mesh):
    link_spec = P(None, *CUTS)
    field_spec = P(*CUTS)
    vmem = pl.BlockSpec(memory_space=pltpu.VMEM)

    def local_solve(fat_links, long_links, source, quark_mass):
        t_len, z_len, y_len, xh_len = source.shape[:4]

        def link_rows(links):
            return jnp.moveaxis(links, 2, -1).reshape(4, t_len, y_len, STRIDE * xh_len, z_len)
        src = jnp.moveaxis(source, 1, -1).reshape(t_len, y_len, COLS * xh_len, z_len)
        hbm = pl.BlockSpec(memory_space=pl.ANY)
        dma = pltpu.SemaphoreType.DMA
        sol, norms = pl.pallas_call(
            cg_kernel,
            out_shape=(jax.ShapeDtypeStruct(src.shape, F32), jax.ShapeDtypeStruct((SUB, LANES), F32)),
            in_specs=[vmem, pl.BlockSpec(memory_space=pltpu.SMEM), hbm, hbm],
            out_specs=(vmem, vmem),
            scratch_shapes=[
                pltpu.VMEM(PP + (288, ROWS, LANES), F32),
                pltpu.VMEM(PP + (COLS, EXT, LANES), F32),
                pltpu.VMEM(PP + (COLS, ROWS, LANES), F32),
                pltpu.VMEM(PP + (ROWS, LANES), F32),
                pltpu.VMEM(PP + (ROWS, LANES), F32),
                pltpu.VMEM((2, COLS, ROWS, LANES), F32),
                pltpu.VMEM((2, COLS, ROWS, LANES), F32),
                pltpu.VMEM((COLS, ROWS, LANES), F32),
                pltpu.VMEM((ROWS, LANES), jnp.int32),
                pltpu.VMEM((ROWS, LANES), jnp.int32),
                pltpu.VMEM((2, SUB, LANES), F32),
                pltpu.VMEM((2, 16, SUB, LANES), F32),
                pltpu.VMEM((5, SUB, LANES), F32),
                pltpu.VMEM((SLOTS, 2, 2, STRIDE * xh_len, z_len), F32),
                pltpu.VMEM((2, 504, LANES), F32),
                pltpu.VMEM((2, COLS, ROWS, LANES), F32),
                pltpu.VMEM((MATS, ROWS, LANES), F32),
                pltpu.VMEM((MATS, ROWS, LANES), F32),
                pltpu.VMEM(PP + (MATS, 16, LANES), F32),
                pltpu.VMEM(PP + (MATS, BASE, LANES), F32),
                pltpu.VMEM(PP + (2, 3, ROWS, LANES), F32),
                pltpu.VMEM(PP + (2, 3, ROWS, LANES), F32),
                *[dma(n) for n in ((SLOTS, 2, 2), (1,), (1,), PP + (2,), PP + (2,))], dma((2,)), dma((2,)),
                dma(PP + (4,)), dma(PP + (4,)), dma((2, DEVS)), dma((2, DEVS)),
            ],
            compiler_params=pltpu.CompilerParams(has_side_effects=True, vmem_limit_bytes=61 * 1024 * 1024),
        )(src, quark_mass, link_rows(fat_links), link_rows(long_links))
        sol = jnp.moveaxis(sol.reshape(t_len, y_len, xh_len, 3, 2, z_len), -1, 1)
        return sol, norms[:, 0]

    return jax.shard_map(local_solve, mesh=mesh, in_specs=(link_spec, link_spec, field_spec, P()), out_specs=(field_spec, P()), check_vma=False)
```
